128 devices in a mesh: dp: 1, sp: 16 (over z, y), tp: 8 (over x, core).
Axes of the slice: x: 4, y: 4, z: 4, core: 2. Of those that a mesh axis runs over, the one named last changes fastest.
Arguments:
- latents: bfloat16 [3, 256, 1280], P('dp')
- queries: bfloat16 [3, 4096, 768], P('dp', 'sp')
- lat_ln1: float32 [1280], replicated
- lat_wq: bfloat16 [1280, 8, 160], P(None, 'tp')
- lat_wk: bfloat16 [1280, 8, 160], P(None, 'tp')
- lat_wv: bfloat16 [1280, 8, 160], P(None, 'tp')
- lat_wo: bfloat16 [8, 160, 1280], P('tp')
- lat_ln2: float32 [1280], replicated
- lat_up: bfloat16 [1280, 1280], P(None, 'tp')
- lat_down: bfloat16 [1280, 1280], P('tp')
- dec_lnq: float32 [768], replicated
- dec_lnkv: float32 [1280], replicated
- dec_wq: bfloat16 [768, 768], replicated
- dec_wk: bfloat16 [1280, 768], replicated
- dec_wv: bfloat16 [1280, 768], replicated
- dec_wo: bfloat16 [768, 768], replicated
- dec_ln: float32 [768], replicated
- dec_up: bfloat16 [768, 768], replicated
- dec_down: bfloat16 [768, 768], replicated
- dec_out: bfloat16 [768, 32000], replicated
Outputs:
- output: bfloat16 [3, 4096, 32000], P('dp', 'sp')
All inputs are finite; a program needn't handle non-finite values.
Results may differ from the reference program's by a relative error of at most 0.02.
Values are sent between devices in bfloat16 or wider.
A program may use at most 1 GiB of HBM per device.

```python
import jax
import jax.numpy as jnp
from jax import lax

BATCH = 3
LATENTS = 256
WIDTH = 1280
HEADS = 8
HEAD_DIM = 160
MLP_WIDTH = 1280
QUERY_CH = 768
DEC_WIDTH = 768
OUT_CH = 32000
QUERIES = 4096
QUERY_BLOCK = 256
LN_EPS = 1e-5


def layer_norm(rows_in, gain_vec):
    widened = rows_in.astype(jnp.float32)
    row_mean = jnp.mean(widened, axis=-1, keepdims=True)
    row_var = jnp.mean(jnp.square(widened - row_mean), axis=-1, keepdims=True)
    return ((widened - row_mean) * lax.rsqrt(row_var + LN_EPS) * gain_vec).astype(jnp.bfloat16)


def setup_inputs(seed: int = 0, part: int = 0) -> dict:
    shared = jax.random.split(jax.random.key(seed), 18)
    own_keys = jax.random.split(jax.random.fold_in(jax.random.key(seed + 1), part), 2)

    def draw_normal(rng_key, arr_shape, std_scale):
        return (jax.random.normal(rng_key, arr_shape, jnp.float32) * std_scale).astype(jnp.bfloat16)

    def draw_gain(rng_key, vec_len):
        return 1.0 + 0.3 * jax.random.normal(rng_key, (vec_len,), jnp.float32)

    head_shape = (WIDTH, HEADS, HEAD_DIM)
    return {
        "latents": draw_normal(own_keys[0], (BATCH, LATENTS, WIDTH), 1.0),
        "queries": draw_normal(own_keys[1], (BATCH, QUERIES, QUERY_CH), 1.0),
        "lat_ln1": draw_gain(shared[0], WIDTH),
        "lat_wq": draw_normal(shared[1], head_shape, 1.5 * WIDTH ** -0.5),
        "lat_wk": draw_normal(shared[2], head_shape, 1.5 * WIDTH ** -0.5),
        "lat_wv": draw_normal(shared[3], head_shape, WIDTH ** -0.5),
        "lat_wo": draw_normal(shared[4], (HEADS, HEAD_DIM, WIDTH), (HEADS * HEAD_DIM) ** -0.5),
        "lat_ln2": draw_gain(shared[5], WIDTH),
        "lat_up": draw_normal(shared[6], (WIDTH, MLP_WIDTH), WIDTH ** -0.5),
        "lat_down": draw_normal(shared[7], (MLP_WIDTH, WIDTH), MLP_WIDTH ** -0.5),
        "dec_lnq": draw_gain(shared[8], QUERY_CH),
        "dec_lnkv": draw_gain(shared[9], WIDTH),
        "dec_wq": draw_normal(shared[10], (QUERY_CH, DEC_WIDTH), 1.5 * QUERY_CH ** -0.5),
        "dec_wk": draw_normal(shared[11], (WIDTH, DEC_WIDTH), 1.5 * WIDTH ** -0.5),
        "dec_wv": draw_normal(shared[12], (WIDTH, DEC_WIDTH), 2.0 * WIDTH ** -0.5),
        "dec_wo": draw_normal(shared[13], (DEC_WIDTH, DEC_WIDTH), 1.5 * DEC_WIDTH ** -0.5),
        "dec_ln": draw_gain(shared[14], DEC_WIDTH),
        "dec_up": draw_normal(shared[15], (DEC_WIDTH, DEC_WIDTH), DEC_WIDTH ** -0.5),
        "dec_down": draw_normal(shared[16], (DEC_WIDTH, DEC_WIDTH), DEC_WIDTH ** -0.5),
        "dec_out": draw_normal(shared[17], (DEC_WIDTH, OUT_CH), DEC_WIDTH ** -0.5),
    }


def latent_layer(z_one, lat_ln1, lat_wq, lat_wk, lat_wv, lat_wo, lat_ln2, lat_up, lat_down):
    normed = layer_norm(z_one, lat_ln1).astype(jnp.float32)
    q_heads = jnp.einsum("nd,dhe->nhe", normed, lat_wq.astype(jnp.float32)).astype(jnp.bfloat16)
    k_heads = jnp.einsum("nd,dhe->nhe", normed, lat_wk.astype(jnp.float32)).astype(jnp.bfloat16)
    v_heads = jnp.einsum("nd,dhe->nhe", normed, lat_wv.astype(jnp.float32)).astype(jnp.bfloat16)
    scores = jnp.einsum("qhe,khe->hqk", q_heads.astype(jnp.float32), k_heads.astype(jnp.float32)) * HEAD_DIM ** -0.5
    attn_probs = jax.nn.softmax(scores, axis=-1).astype(jnp.bfloat16)
    context = jnp.einsum("hqk,khe->qhe", attn_probs.astype(jnp.float32), v_heads.astype(jnp.float32)).astype(jnp.bfloat16)
    attn_out = jnp.einsum("qhe,hed->qd", context.astype(jnp.float32), lat_wo.astype(jnp.float32))
    z_mid = (z_one.astype(jnp.float32) + attn_out).astype(jnp.bfloat16)
    hidden = jax.nn.gelu(jnp.dot(layer_norm(z_mid, lat_ln2), lat_up, preferred_element_type=jnp.float32), approximate=False).astype(jnp.bfloat16)
    return (z_mid.astype(jnp.float32) + jnp.dot(hidden, lat_down, preferred_element_type=jnp.float32)).astype(jnp.bfloat16)


def decode_block(q_block, all_keys, all_values, dec_lnq, dec_wq, dec_wo, dec_ln, dec_up, dec_down, dec_out):
    q_proj = jnp.dot(layer_norm(q_block, dec_lnq), dec_wq, preferred_element_type=jnp.float32).astype(jnp.bfloat16)
    scores = jnp.dot(q_proj, all_keys.T, preferred_element_type=jnp.float32) * DEC_WIDTH ** -0.5
    attn_probs = jax.nn.softmax(scores, axis=-1).astype(jnp.bfloat16)
    context = jnp.dot(attn_probs, all_values, preferred_element_type=jnp.float32).astype(jnp.bfloat16)
    mixed_rows = (q_proj.astype(jnp.float32) + jnp.dot(context, dec_wo, preferred_element_type=jnp.float32)).astype(jnp.bfloat16)
    hidden = jax.nn.gelu(jnp.dot(layer_norm(mixed_rows, dec_ln), dec_up, preferred_element_type=jnp.float32), approximate=False).astype(jnp.bfloat16)
    final_rows = (mixed_rows.astype(jnp.float32) + jnp.dot(hidden, dec_down, preferred_element_type=jnp.float32)).astype(jnp.bfloat16)
    return jnp.dot(final_rows, dec_out, preferred_element_type=jnp.float32).astype(jnp.bfloat16)


def reference(latents, queries, lat_ln1, lat_wq, lat_wk, lat_wv, lat_wo, lat_ln2, lat_up, lat_down, dec_lnq, dec_lnkv, dec_wq, dec_wk, dec_wv, dec_wo, dec_ln, dec_up, dec_down, dec_out):
    def one_item(item_pair):
        z_one, q_one = item_pair
        z_new = latent_layer(z_one, lat_ln1, lat_wq, lat_wk, lat_wv, lat_wo, lat_ln2, lat_up, lat_down)
        kv_in = layer_norm(z_new, dec_lnkv)
        all_keys = jnp.dot(kv_in, dec_wk, preferred_element_type=jnp.float32).astype(jnp.bfloat16)
        all_values = jnp.dot(kv_in, dec_wv, preferred_element_type=jnp.float32).astype(jnp.bfloat16)
        query_blocks = q_one.reshape(QUERIES // QUERY_BLOCK, QUERY_BLOCK, QUERY_CH)
        out_blocks = lax.map(lambda q_block: decode_block(q_block, all_keys, all_values, dec_lnq, dec_wq, dec_wo, dec_ln, dec_up, dec_down, dec_out), query_blocks)
        return out_blocks.reshape(QUERIES, OUT_CH)
    return lax.map(one_item, (latents, queries))
```

```python
import jax
import jax.numpy as jnp
from jax import lax
from jax.sharding import PartitionSpec as P

LN_EPS = 1e-5


def layer_norm(rows_in, gain_vec):
    widened = rows_in.astype(jnp.float32)
    row_mean = jnp.mean(widened, axis=-1, keepdims=True)
    row_var = jnp.mean(jnp.square(widened - row_mean), axis=-1, keepdims=True)
    return ((widened - row_mean) * lax.rsqrt(row_var + LN_EPS) * gain_vec).astype(jnp.bfloat16)


def decode_rows(query_rows, all_keys, all_values, dec_lnq, dec_wq, dec_wo, dec_ln, dec_up, dec_down, dec_out):
    q_proj = jnp.dot(layer_norm(query_rows, dec_lnq), dec_wq, preferred_element_type=jnp.float32).astype(jnp.bfloat16)
    scores = jnp.einsum("crd,cld->crl", q_proj, all_keys, preferred_element_type=jnp.float32) * dec_wq.shape[1] ** -0.5
    attn_probs = jax.nn.softmax(scores, axis=-1).astype(jnp.bfloat16)
    context = jnp.einsum("crl,cld->crd", attn_probs, all_values, preferred_element_type=jnp.float32).astype(jnp.bfloat16)
    mixed_rows = (q_proj.astype(jnp.float32) + jnp.dot(context, dec_wo, preferred_element_type=jnp.float32)).astype(jnp.bfloat16)
    hidden = jax.nn.gelu(jnp.dot(layer_norm(mixed_rows, dec_ln), dec_up, preferred_element_type=jnp.float32), approximate=False).astype(jnp.bfloat16)
    final_rows = (mixed_rows.astype(jnp.float32) + jnp.dot(hidden, dec_down, preferred_element_type=jnp.float32)).astype(jnp.bfloat16)
    return jnp.dot(final_rows, dec_out, preferred_element_type=jnp.float32).astype(jnp.bfloat16)


def solution(mesh):
    head_split = P(None, "tp", None)
    whole_vec = P(None)
    whole_mat = P(None, None)
    in_specs = (P("dp", None, None), P("dp", "sp", None), whole_vec, head_split, head_split, head_split, P("tp", None, None), whole_vec, P(None, "tp"), P("tp", None), whole_vec, whole_vec, whole_mat, whole_mat, whole_mat, whole_mat, whole_vec, whole_mat, whole_mat, whole_mat)

    def local_step(latents, queries, lat_ln1, lat_wq, lat_wk, lat_wv, lat_wo, lat_ln2, lat_up, lat_down, dec_lnq, dec_lnkv, dec_wq, dec_wk, dec_wv, dec_wo, dec_ln, dec_up, dec_down, dec_out):
        tp_index = lax.axis_index("tp")
        head_dim = lat_wq.shape[2]
        normed = layer_norm(latents, lat_ln1)
        q_heads = jnp.einsum("bnd,dhe->bnhe", normed, lat_wq, preferred_element_type=jnp.float32).astype(jnp.bfloat16)
        k_heads = jnp.einsum("bnd,dhe->bnhe", normed, lat_wk, preferred_element_type=jnp.float32).astype(jnp.bfloat16)
        v_heads = jnp.einsum("bnd,dhe->bnhe", normed, lat_wv, preferred_element_type=jnp.float32).astype(jnp.bfloat16)
        scores = jnp.einsum("bqhe,bkhe->bhqk", q_heads, k_heads, preferred_element_type=jnp.float32) * head_dim ** -0.5
        attn_probs = jax.nn.softmax(scores, axis=-1).astype(jnp.bfloat16)
        context = jnp.einsum("bhqk,bkhe->bqhe", attn_probs, v_heads, preferred_element_type=jnp.float32).astype(jnp.bfloat16)
        attn_part = jnp.einsum("crif,ife->cre", context, lat_wo, preferred_element_type=jnp.float32).astype(jnp.bfloat16)
        attn_sum = lax.psum(attn_part, "tp")
        z_mid = (latents.astype(jnp.float32) + attn_sum.astype(jnp.float32)).astype(jnp.bfloat16)
        hidden = jax.nn.gelu(jnp.dot(layer_norm(z_mid, lat_ln2), lat_up, preferred_element_type=jnp.float32), approximate=False).astype(jnp.bfloat16)
        mlp_part = jnp.dot(hidden, lat_down, preferred_element_type=jnp.float32).astype(jnp.bfloat16)
        mlp_rows = lax.psum_scatter(mlp_part, "tp", scatter_dimension=1, tiled=True)
        row_count = mlp_rows.shape[1]
        mid_rows = lax.dynamic_slice_in_dim(z_mid, tp_index * row_count, row_count, axis=1)
        new_rows = (mid_rows.astype(jnp.float32) + mlp_rows.astype(jnp.float32)).astype(jnp.bfloat16)
        kv_in = layer_norm(new_rows, dec_lnkv)
        key_rows = jnp.dot(kv_in, dec_wk, preferred_element_type=jnp.float32).astype(jnp.bfloat16)
        value_rows = jnp.dot(kv_in, dec_wv, preferred_element_type=jnp.float32).astype(jnp.bfloat16)
        all_keys = lax.all_gather(key_rows, "tp", axis=1, tiled=True)
        all_values = lax.all_gather(value_rows, "tp", axis=1, tiled=True)
        return decode_rows(queries, all_keys, all_values, dec_lnq, dec_wq, dec_wo, dec_ln, dec_up, dec_down, dec_out)

    return jax.shard_map(local_step, mesh=mesh, in_specs=in_specs, out_specs=P("dp", "sp", None), check_vma=False)
```

```python
import functools

import jax
import jax.numpy as jnp
from jax import lax
from jax.experimental import pallas as pl
from jax.experimental.pallas import tpu as pltpu
from jax.sharding import PartitionSpec as P

LN_EPS = 1e-5
MESH = pl.DeviceIdType.MESH
F32 = jnp.float32
BF16 = jnp.bfloat16


def norm_rows(widened, gain_row):
    row_mean = jnp.mean(widened, axis=-1, keepdims=True)
    centred = widened - row_mean
    row_var = jnp.mean(jnp.square(centred), axis=-1, keepdims=True)
    return (centred * lax.rsqrt(row_var + LN_EPS) * gain_row).astype(BF16)


def gelu(val):
    return 0.5 * val * (1.0 + lax.erf(val * (0.5**0.5)))


def dot(lhs, rhs):
    return jnp.dot(lhs, rhs, preferred_element_type=F32)


def dot_t(lhs, rhs):
    return lax.dot_general(lhs, rhs, (((1,), (1,)), ((), ())), preferred_element_type=F32)


def softmax(scores):
    shifted = jnp.exp(scores - jnp.max(scores, axis=-1, keepdims=True))
    return (shifted / jnp.sum(shifted, axis=-1, keepdims=True)).astype(BF16)


def front_kernel(
    z_hbm, q_hbm, wq_hbm, wk_hbm, wv_hbm, wo_hbm, up_hbm, down_hbm, dwq_hbm, dwk_hbm, dwv_hbm, dwo_hbm, dup_hbm, ddn_hbm,
    g1, g2, gq, gkv, gd,
    x2_hbm,
    z, zr, wqkv, wrest, queries, dwq, dwk, dwv, dwo, dup, ddn,
    normed, khead, vhead, part1, part2, kbuf, vbuf, qd, x2,
    load_sem, out_sem, pair_sem, x_sem, k1_sem, v1_sem, k2_sem, v2_sem, k3_sem, v3_sem,
):
    sp, tp = lax.axis_index("sp"), lax.axis_index("tp")
    zc, yc = sp // 4, sp % 4
    xc, core = tp // 2, tp % 2
    items, latents, width = z.shape
    rows = items * 8

    partner = {"tp": tp + 1 - 2 * core}
    x_peer = [{"tp": ((xc + d) % 4) * 2 + core} for d in (1, 2, 3)]
    y_peer = [{"sp": zc * 4 + (yc + d) % 4} for d in (1, 2, 3)]
    z_peer = [{"sp": ((zc + d) % 4) * 4 + yc} for d in (1, 2, 3)]

    def remote(src, dst, sems, where):
        copy = pltpu.make_async_remote_copy(
            src_ref=src, dst_ref=dst, send_sem=sems.at[0], recv_sem=sems.at[1], device_id=where, device_id_type=MESH)
        copy.start()
        return copy

    barrier = pltpu.get_barrier_semaphore()
    peers = [partner] + x_peer + y_peer + z_peer
    for peer in peers:
        pl.semaphore_signal(barrier, inc=1, device_id=peer, device_id_type=MESH)

    loads = []

    def load(src, dst):
        copy = pltpu.make_async_copy(src, dst, load_sem.at[len(loads)])
        copy.start()
        loads.append(copy)
        return copy

    load_q = [load(src, wqkv.at[0, i]) for i, src in enumerate((wq_hbm, wk_hbm, wv_hbm))]
    load_z = load(z_hbm, z)
    load_zr = load(z_hbm.at[:, pl.ds(pl.multiple_of(sp * 16 + core * 8, 8), 8), :], zr)
    load_r = [load(src, wrest.at[0, i]) for i, src in enumerate((wo_hbm, up_hbm, down_hbm))]
    load_dq = [load(q_hbm, queries), load(dwq_hbm, dwq)]
    load_kv = [load(dwk_hbm, dwk), load(dwv_hbm, dwv)]
    load_dec = [load(dwo_hbm, dwo), load(dup_hbm, dup), load(ddn_hbm, ddn)]

    for copy in load_q:
        copy.wait()
    pl.semaphore_wait(barrier, len(peers))
    swap_q = remote(wqkv.at[0], wqkv.at[1], pair_sem.at[0], partner)
    for copy in load_r:
        copy.wait()
    swap_r = remote(wrest.at[0], wrest.at[1], pair_sem.at[1], partner)

    load_z.wait()
    for b in range(items):
        def norm_step(i, carry, b=b):
            at = pl.multiple_of(i * 32, 32)
            normed[pl.ds(pl.multiple_of(b * latents + at, 32), 32), :] = norm_rows(z[b, pl.ds(at, 32), :].astype(F32), g1[...])
            return carry
        lax.fori_loop(0, latents // 32, norm_step, 0)
    load_zr.wait()
    z_rows = zr[...].astype(F32).reshape(rows, width)
    normed_rows = norm_rows(z_rows, g1[...])

    attn = jnp.zeros((rows, width), F32)
    for h in range(2):
        if h == 1:
            swap_q.wait_recv()
        q_rows = dot_t(normed_rows, wqkv[h, 0]).astype(BF16)
        khead[...] = dot_t(normed[...], wqkv[h, 1]).astype(BF16)
        vhead[...] = dot_t(normed[...], wqkv[h, 2]).astype(BF16)
        wide = dot_t(q_rows, khead[...])
        scores = jnp.concatenate([wide[8 * b : 8 * b + 8, latents * b : latents * (b + 1)] for b in range(items)], axis=0)
        probs = softmax(scores * q_rows.shape[1] ** -0.5)
        context = jnp.concatenate(
            [dot(probs, vhead[latents * b : latents * (b + 1), :])[8 * b : 8 * b + 8] for b in range(items)], axis=0).astype(BF16)
        if h == 1:
            swap_r.wait_recv()
        attn = attn + dot(context, wrest[h, 0])
    part1[xc] = attn.astype(BF16)
    sent1 = [remote(part1.at[xc], part1.at[xc], x_sem.at[0, d], x_peer[d]) for d in range(3)]

    for copy in load_dq:
        copy.wait()
    for b in range(items):
        at = latents * b
        qd[at : at + latents, :] = dot(norm_rows(queries[b].astype(F32), gq[...]), dwq[...]).astype(BF16)

    for copy in sent1:
        copy.wait_recv()
    total = part1[0].astype(F32)
    for s in range(1, 4):
        total = total + part1[s].astype(F32)
    z_mid = (z_rows + total).astype(BF16)
    normed_mid = norm_rows(z_mid.astype(F32), g2[...])
    mlp = jnp.zeros((rows, width), F32)
    for h in range(2):
        hidden = gelu(dot_t(normed_mid, wrest[h, 1])).astype(BF16)
        mlp = mlp + dot(hidden, wrest[h, 2])
    part2[xc] = mlp.astype(BF16)
    sent2 = [remote(part2.at[xc], part2.at[xc], x_sem.at[1, d], x_peer[d]) for d in range(3)]

    for copy in load_kv:
        copy.wait()
    for copy in sent2:
        copy.wait_recv()
    total = part2[0].astype(F32)
    for s in range(1, 4):
        total = total + part2[s].astype(F32)
    z_new = (z_mid.astype(F32) + total).astype(BF16)
    kv_in = norm_rows(z_new.astype(F32), gkv[...])
    for b_, (buf, wt) in enumerate(((kbuf, dwk), (vbuf, dwv))):
        val = dot(kv_in, wt[...])
        for b in range(items):
            buf[b, core, zc, yc] = val[8 * b : 8 * b + 8].astype(BF16)

    k1 = [[remote(kbuf.at[b, core, zc, yc], kbuf.at[b, core, zc, yc], k1_sem.at[b, d], y_peer[d]) for d in range(3)] for b in range(items)]
    v1 = [[remote(vbuf.at[b, core, zc, yc], vbuf.at[b, core, zc, yc], v1_sem.at[b, d], z_peer[d]) for d in range(3)] for b in range(items)]
    for copy in load_dec:
        copy.wait()
    k2, v2, k3, v3 = [], [], [], []
    for b in range(items):
        for copy in k1[b]:
            copy.wait_recv()
        k2.append([remote(kbuf.at[b, core, zc], kbuf.at[b, core, zc], k2_sem.at[b, d], z_peer[d]) for d in range(3)])
        for copy in v1[b]:
            copy.wait_recv()
        v2.append([remote(vbuf.at[b, core, :, yc], vbuf.at[b, core, :, yc], v2_sem.at[b, d], y_peer[d]) for d in range(3)])

    def swap(b):
        for copy in k2[b]:
            copy.wait_recv()
        k3.append(remote(kbuf.at[b, core], kbuf.at[b, core], k3_sem.at[b], partner))
        for copy in v2[b]:
            copy.wait_recv()
        v3.append(remote(vbuf.at[b, core], vbuf.at[b, core], v3_sem.at[b], partner))

    stores = []

    def decode(b):
        at = latents * b
        channels = qd.shape[1]
        q_item = qd[at : at + latents, :]
        k3[b].wait_recv()
        keys = kbuf[b].astype(F32).reshape(latents, channels).astype(BF16)
        probs = softmax(dot_t(q_item, keys) * channels**-0.5)
        v3[b].wait_recv()
        values = vbuf[b].astype(F32).reshape(latents, channels).astype(BF16)
        context = dot(probs, values).astype(BF16)
        mixed = (q_item.astype(F32) + dot(context, dwo[...])).astype(BF16)
        hidden = gelu(dot(norm_rows(mixed.astype(F32), gd[...]), dup[...])).astype(BF16)
        x2[at : at + latents, :] = (mixed.astype(F32) + dot(hidden, ddn[...])).astype(BF16)
        store = pltpu.make_async_copy(x2.at[at : at + latents], x2_hbm.at[at : at + latents], out_sem.at[b])
        store.start()
        stores.append(store)

    swap(0)
    swap(1)
    decode(0)
    swap(2)
    decode(1)
    decode(2)

    for copy in [swap_q, swap_r] + sent1 + sent2 + sum(k1 + v1 + k2 + v2, []) + k3 + v3:
        copy.wait_send()
    for store in stores:
        store.wait()


def front(latents, queries, lat_ws, dec_ws, gains):
    items, lat_rows, width = latents.shape
    channels = queries.shape[2]
    head = lat_ws[0].shape[0]
    anywhere = pl.BlockSpec(memory_space=pl.ANY)
    vmem = pl.BlockSpec(memory_space=pltpu.VMEM)
    total = items * lat_rows
    dma = pltpu.SemaphoreType.DMA
    return pl.pallas_call(
        front_kernel,
        out_shape=jax.ShapeDtypeStruct((total, channels), BF16),
        in_specs=[anywhere] * 14 + [vmem] * 5,
        out_specs=anywhere,
        scratch_shapes=[
            pltpu.VMEM((items, lat_rows, width), BF16),
            pltpu.VMEM((items, 8, width), BF16),
            pltpu.VMEM((2, 3, head, width), BF16),
            pltpu.VMEM((2, 3, head, width), BF16),
            pltpu.VMEM((items, lat_rows, channels), BF16),
            pltpu.VMEM((channels, channels), BF16),
            pltpu.VMEM((width, channels), BF16),
            pltpu.VMEM((width, channels), BF16),
            pltpu.VMEM((channels, channels), BF16),
            pltpu.VMEM((channels, channels), BF16),
            pltpu.VMEM((channels, channels), BF16),
            pltpu.VMEM((total, width), BF16),
            pltpu.VMEM((total, head), BF16),
            pltpu.VMEM((total, head), BF16),
            pltpu.VMEM((4, items * 8, width), BF16),
            pltpu.VMEM((4, items * 8, width), BF16),
            pltpu.VMEM((items, 2, 4, 4, 8, channels), BF16),
            pltpu.VMEM((items, 2, 4, 4, 8, channels), BF16),
            pltpu.VMEM((total, channels), BF16),
            pltpu.VMEM((total, channels), BF16),
            dma((15,)),
            dma((items,)),
            dma((2, 2)),
            dma((2, 3, 2)),
            dma((items, 3, 2)),
            dma((items, 3, 2)),
            dma((items, 3, 2)),
            dma((items, 3, 2)),
            dma((items, 2)),
            dma((items, 2)),
        ],
        compiler_params=pltpu.CompilerParams(collective_id=0, has_side_effects=True, vmem_limit_bytes=48 * 2**20),
        name="front",
    )(latents, queries, *lat_ws, *dec_ws, *gains)


def out_kernel(x2, wt, out):
    for at in range(0, x2.shape[0], 256):
        out[at : at + 256, :] = dot(x2[at : at + 256, :], wt[...]).astype(BF16)


def out_product(x2, dec_out):
    rows, channels = x2.shape
    cols = dec_out.shape[1]
    tile = 3200
    return pl.pallas_call(
        out_kernel,
        grid=(cols // tile,),
        in_specs=[pl.BlockSpec((rows, channels), lambda i: (0, 0)), pl.BlockSpec((channels, tile), lambda i: (0, i))],
        out_specs=pl.BlockSpec((rows, tile), lambda i: (0, i)),
        out_shape=jax.ShapeDtypeStruct((rows, cols), BF16),
        compiler_params=pltpu.CompilerParams(vmem_limit_bytes=56 * 2**20),
        name="out_product",
    )(x2, dec_out)


def solution(mesh):
    head_split = P(None, "tp", None)
    whole_vec = P(None)
    whole_mat = P(None, None)
    in_specs = (P("dp", None, None), P("dp", "sp", None), whole_vec, head_split, head_split, head_split, P("tp", None, None), whole_vec, P(None, "tp"), P("tp", None), whole_vec, whole_vec, whole_mat, whole_mat, whole_mat, whole_mat, whole_vec, whole_mat, whole_mat, whole_mat)

    def local_step(latents, queries, lat_ln1, lat_wq, lat_wk, lat_wv, lat_wo, lat_ln2, lat_up, lat_down, dec_lnq, dec_lnkv, dec_wq, dec_wk, dec_wv, dec_wo, dec_ln, dec_up, dec_down, dec_out):
        lat_ws = [wt[:, 0, :].T for wt in (lat_wq, lat_wk, lat_wv)] + [lat_wo[0], lat_up.T, lat_down]
        gains = [gain[None, :] for gain in (lat_ln1, lat_ln2, dec_lnq, dec_lnkv, dec_ln)]
        x2 = front(latents, queries, lat_ws, [dec_wq, dec_wk, dec_wv, dec_wo, dec_up, dec_down], gains)
        out = out_product(x2, dec_out)
        return out.reshape(queries.shape[0], queries.shape[1], dec_out.shape[1])

    return jax.shard_map(local_step, mesh=mesh, in_specs=in_specs, out_specs=P("dp", "sp", None), check_vma=False)
```

```python
import functools

import jax
import jax.numpy as jnp
from jax import lax
from jax.experimental import pallas as pl
from jax.experimental.pallas import tpu as pltpu
from jax.sharding import PartitionSpec as P

LN_EPS = 1e-5
MESH = pl.DeviceIdType.MESH
F32 = jnp.float32
BF16 = jnp.bfloat16
VMEM_BYTES = 67043328


def norm_rows(widened, gain_row):
    row_mean = jnp.mean(widened, axis=-1, keepdims=True)
    centred = widened - row_mean
    row_var = jnp.mean(jnp.square(centred), axis=-1, keepdims=True)
    return (centred * lax.rsqrt(row_var + LN_EPS) * gain_row).astype(BF16)


def gelu(val):
    return 0.5 * val * (1.0 + lax.erf(val * (0.5**0.5)))


def dot(lhs, rhs):
    return jnp.dot(lhs, rhs, preferred_element_type=F32)


def dot_t(lhs, rhs):
    return lax.dot_general(lhs, rhs, (((1,), (1,)), ((), ())), preferred_element_type=F32)


def softmax(scores):
    shifted = jnp.exp(scores - jnp.max(scores, axis=-1, keepdims=True))
    return (shifted / jnp.sum(shifted, axis=-1, keepdims=True)).astype(BF16)


def front_kernel(
    z_hbm, q_hbm, wq_hbm, wk_hbm, wv_hbm, wo_hbm, up_hbm, down_hbm, dwq_hbm, dwk_hbm, dwv_hbm, dwo_hbm, dup_hbm, ddn_hbm,
    g1_hbm, g2_hbm, gq_hbm, gkv_hbm, gd_hbm,
    x2_hbm,
    z, zr, wqkv, wrest, queries, dwq, dwk, dwv, dwo, dup, ddn,
    g1, g2, gq, gkv, gd, normed, khead, vhead, part1, part2, kbuf, vbuf, qd, x2,
    load_sem, out_sem, pair_sem, x_sem, k1_sem, v1_sem, k2_sem, v2_sem, k3_sem, v3_sem,
):
    sp, tp = lax.axis_index("sp"), lax.axis_index("tp")
    zc, yc = sp // 4, sp % 4
    xc, core = tp // 2, tp % 2
    items, latents, width = z.shape
    rows = items * 8

    partner = {"tp": tp + 1 - 2 * core}
    x_peer = [{"tp": ((xc + d) % 4) * 2 + core} for d in (1, 2, 3)]
    y_peer = [{"sp": zc * 4 + (yc + d) % 4} for d in (1, 2, 3)]
    z_peer = [{"sp": ((zc + d) % 4) * 4 + yc} for d in (1, 2, 3)]

    def remote(src, dst, sems, where):
        copy = pltpu.make_async_remote_copy(
            src_ref=src, dst_ref=dst, send_sem=sems.at[0], recv_sem=sems.at[1], device_id=where, device_id_type=MESH)
        copy.start()
        return copy

    barrier = pltpu.get_barrier_semaphore()
    peers = [partner] + x_peer + y_peer + z_peer
    for peer in peers:
        pl.semaphore_signal(barrier, inc=1, device_id=peer, device_id_type=MESH)

    loads = []

    def load(src, dst):
        copy = pltpu.make_async_copy(src, dst, load_sem.at[len(loads)])
        copy.start()
        loads.append(copy)
        return copy

    load_g = [load(src, dst) for src, dst in ((g1_hbm, g1), (g2_hbm, g2), (gq_hbm, gq), (gkv_hbm, gkv), (gd_hbm, gd))]
    load_q = [load(src, wqkv.at[0, i]) for i, src in enumerate((wq_hbm, wk_hbm, wv_hbm))]
    load_z = load(z_hbm, z)
    load_zr = load(z_hbm.at[:, pl.ds(pl.multiple_of(sp * 16 + core * 8, 8), 8), :], zr)
    load_r = [load(src, wrest.at[0, i]) for i, src in enumerate((wo_hbm, up_hbm, down_hbm))]
    load_dq = [load(q_hbm, queries), load(dwq_hbm, dwq)]
    load_kv = [load(dwk_hbm, dwk), load(dwv_hbm, dwv)]
    load_dec = [load(dwo_hbm, dwo), load(dup_hbm, dup), load(ddn_hbm, ddn)]

    for copy in load_g + load_q:
        copy.wait()
    pl.semaphore_wait(barrier, len(peers))
    swap_q = remote(wqkv.at[0], wqkv.at[1], pair_sem.at[0], partner)
    for copy in load_r:
        copy.wait()
    swap_r = remote(wrest.at[0], wrest.at[1], pair_sem.at[1], partner)

    load_z.wait()
    for b in range(items):
        def norm_step(i, carry, b=b):
            at = pl.multiple_of(i * 32, 32)
            normed[pl.ds(pl.multiple_of(b * latents + at, 32), 32), :] = norm_rows(z[b, pl.ds(at, 32), :].astype(F32), g1[...])
            return carry
        lax.fori_loop(0, latents // 32, norm_step, 0)
    load_zr.wait()
    z_rows = zr[...].astype(F32).reshape(rows, width)
    normed_rows = norm_rows(z_rows, g1[...])

    attn = jnp.zeros((rows, width), F32)
    for h in range(2):
        if h == 1:
            swap_q.wait_recv()
        q_rows = dot_t(normed_rows, wqkv[h, 0]).astype(BF16)
        khead[...] = dot_t(normed[...], wqkv[h, 1]).astype(BF16)
        vhead[...] = dot_t(normed[...], wqkv[h, 2]).astype(BF16)
        wide = dot_t(q_rows, khead[...])
        scores = jnp.concatenate([wide[8 * b : 8 * b + 8, latents * b : latents * (b + 1)] for b in range(items)], axis=0)
        probs = softmax(scores * q_rows.shape[1] ** -0.5)
        context = jnp.concatenate(
            [dot(probs, vhead[latents * b : latents * (b + 1), :])[8 * b : 8 * b + 8] for b in range(items)], axis=0).astype(BF16)
        if h == 1:
            swap_r.wait_recv()
        attn = attn + dot(context, wrest[h, 0])
    part1[xc] = attn.astype(BF16)
    sent1 = [remote(part1.at[xc], part1.at[xc], x_sem.at[0, d], x_peer[d]) for d in range(3)]

    for copy in load_dq:
        copy.wait()
    for b in range(items):
        at = latents * b
        qd[at : at + latents, :] = dot(norm_rows(queries[b].astype(F32), gq[...]), dwq[...]).astype(BF16)

    for copy in sent1:
        copy.wait_recv()
    total = part1[0].astype(F32)
    for s in range(1, 4):
        total = total + part1[s].astype(F32)
    z_mid = (z_rows + total).astype(BF16)
    normed_mid = norm_rows(z_mid.astype(F32), g2[...])
    mlp = jnp.zeros((rows, width), F32)
    for h in range(2):
        hidden = gelu(dot_t(normed_mid, wrest[h, 1])).astype(BF16)
        mlp = mlp + dot(hidden, wrest[h, 2])
    part2[xc] = mlp.astype(BF16)
    sent2 = [remote(part2.at[xc], part2.at[xc], x_sem.at[1, d], x_peer[d]) for d in range(3)]

    for copy in load_kv:
        copy.wait()
    for copy in sent2:
        copy.wait_recv()
    total = part2[0].astype(F32)
    for s in range(1, 4):
        total = total + part2[s].astype(F32)
    z_new = (z_mid.astype(F32) + total).astype(BF16)
    kv_in = norm_rows(z_new.astype(F32), gkv[...])
    for b_, (buf, wt) in enumerate(((kbuf, dwk), (vbuf, dwv))):
        val = dot(kv_in, wt[...])
        for b in range(items):
            buf[b, core, zc, yc] = val[8 * b : 8 * b + 8].astype(BF16)

    k1 = [[remote(kbuf.at[b, core, zc, yc], kbuf.at[b, core, zc, yc], k1_sem.at[b, d], y_peer[d]) for d in range(3)] for b in range(items)]
    v1 = [[remote(vbuf.at[b, core, zc, yc], vbuf.at[b, core, zc, yc], v1_sem.at[b, d], z_peer[d]) for d in range(3)] for b in range(items)]
    for copy in load_dec:
        copy.wait()
    k2, v2, k3, v3 = [], [], [], []
    for b in range(items):
        for copy in k1[b]:
            copy.wait_recv()
        k2.append([remote(kbuf.at[b, core, zc], kbuf.at[b, core, zc], k2_sem.at[b, d], z_peer[d]) for d in range(3)])
        for copy in v1[b]:
            copy.wait_recv()
        v2.append([remote(vbuf.at[b, core, :, yc], vbuf.at[b, core, :, yc], v2_sem.at[b, d], y_peer[d]) for d in range(3)])

    def swap(b):
        for copy in k2[b]:
            copy.wait_recv()
        k3.append(remote(kbuf.at[b, core], kbuf.at[b, core], k3_sem.at[b], partner))
        for copy in v2[b]:
            copy.wait_recv()
        v3.append(remote(vbuf.at[b, core], vbuf.at[b, core], v3_sem.at[b], partner))

    stores = []

    def decode(b):
        at = latents * b
        channels = qd.shape[1]
        q_item = qd[at : at + latents, :]
        k3[b].wait_recv()
        keys = kbuf[b].astype(F32).reshape(latents, channels).astype(BF16)
        probs = softmax(dot_t(q_item, keys) * channels**-0.5)
        v3[b].wait_recv()
        values = vbuf[b].astype(F32).reshape(latents, channels).astype(BF16)
        context = dot(probs, values).astype(BF16)
        mixed = (q_item.astype(F32) + dot(context, dwo[...])).astype(BF16)
        hidden = gelu(dot(norm_rows(mixed.astype(F32), gd[...]), dup[...])).astype(BF16)
        x2[at : at + latents, :] = (mixed.astype(F32) + dot(hidden, ddn[...])).astype(BF16)
        store = pltpu.make_async_copy(x2.at[at : at + latents], x2_hbm.at[at : at + latents], out_sem.at[b])
        store.start()
        stores.append(store)

    swap(0)
    swap(1)
    decode(0)
    swap(2)
    decode(1)
    decode(2)

    for copy in [swap_q, swap_r] + sent1 + sent2 + sum(k1 + v1 + k2 + v2, []) + k3 + v3:
        copy.wait_send()
    for store in stores:
        store.wait()


def front(latents, queries, lat_ws, dec_ws, gains):
    items, lat_rows, width = latents.shape
    channels = queries.shape[2]
    head = lat_ws[0].shape[0]
    anywhere = pl.BlockSpec(memory_space=pl.ANY)
    total = items * lat_rows
    dma = pltpu.SemaphoreType.DMA
    return pl.pallas_call(
        front_kernel,
        out_shape=jax.ShapeDtypeStruct((total, channels), BF16),
        in_specs=[anywhere] * 19,
        out_specs=anywhere,
        scratch_shapes=[
            pltpu.VMEM((items, lat_rows, width), BF16),
            pltpu.VMEM((items, 8, width), BF16),
            pltpu.VMEM((2, 3, head, width), BF16),
            pltpu.VMEM((2, 3, head, width), BF16),
            pltpu.VMEM((items, lat_rows, channels), BF16),
            pltpu.VMEM((channels, channels), BF16),
            pltpu.VMEM((width, channels), BF16),
            pltpu.VMEM((width, channels), BF16),
            pltpu.VMEM((channels, channels), BF16),
            pltpu.VMEM((channels, channels), BF16),
            pltpu.VMEM((channels, channels), BF16),
            pltpu.VMEM((width,), F32),
            pltpu.VMEM((width,), F32),
            pltpu.VMEM((channels,), F32),
            pltpu.VMEM((width,), F32),
            pltpu.VMEM((channels,), F32),
            pltpu.VMEM((total, width), BF16),
            pltpu.VMEM((total, head), BF16),
            pltpu.VMEM((total, head), BF16),
            pltpu.VMEM((4, items * 8, width), BF16),
            pltpu.VMEM((4, items * 8, width), BF16),
            pltpu.VMEM((items, 2, 4, 4, 8, channels), BF16),
            pltpu.VMEM((items, 2, 4, 4, 8, channels), BF16),
            pltpu.VMEM((total, channels), BF16),
            pltpu.VMEM((total, channels), BF16),
            dma((20,)),
            dma((items,)),
            dma((2, 2)),
            dma((2, 3, 2)),
            dma((items, 3, 2)),
            dma((items, 3, 2)),
            dma((items, 3, 2)),
            dma((items, 3, 2)),
            dma((items, 2)),
            dma((items, 2)),
        ],
        compiler_params=pltpu.CompilerParams(collective_id=0, has_side_effects=True, vmem_limit_bytes=VMEM_BYTES),
        name="front",
    )(latents, queries, *lat_ws, *dec_ws, *gains)


def out_kernel(x2_hbm, wt_hbm, out_hbm, x2, wt, out, x2_sem, wt_sem, out_sem):
    cols = out_hbm.shape[1]
    slots, _, tile = wt.shape
    steps, rest = cols // tile, cols % tile

    def fetch(i, slot, size=tile):
        at = pl.multiple_of(i * tile, tile)
        return pltpu.make_async_copy(wt_hbm.at[:, pl.ds(at, size)], wt.at[slot, :, :size], wt_sem.at[slot])

    def store(i, slot, size=tile):
        at = pl.multiple_of(i * tile, tile)
        return pltpu.make_async_copy(out.at[slot, :, :size], out_hbm.at[:, pl.ds(at, size)], out_sem.at[slot])

    def product(slot, size):
        for at in range(0, x2.shape[0], 256):
            out[slot, at : at + 256, :size] = dot(x2[at : at + 256, :], wt[slot, :, :size]).astype(BF16)

    load_x2 = pltpu.make_async_copy(x2_hbm, x2, x2_sem)
    load_x2.start()
    for i in range(slots):
        fetch(i, i).start()
    load_x2.wait()

    def step(i, carry):
        slot = i % slots
        fetch(i, slot).wait()

        @pl.when(i >= slots)
        def _():
            store(i - slots, slot).wait()

        product(slot, tile)
        store(i, slot).start()

        @pl.when(i + slots < steps)
        def _():
            fetch(i + slots, slot).start()

        @pl.when(i + slots == steps)
        def _():
            fetch(steps, slot, rest).start()

        return carry

    lax.fori_loop(0, steps, step, 0)
    last = steps % slots
    fetch(steps, last, rest).wait()
    store(steps - slots, last).wait()
    product(last, rest)
    store(steps, last, rest).start()
    for i in range(steps - slots + 1, steps):
        store(i, i % slots).wait()
    store(steps, last, rest).wait()


def out_product(x2, dec_out):
    rows, channels = x2.shape
    cols = dec_out.shape[1]
    tile, slots = 2048, 3
    anywhere = pl.BlockSpec(memory_space=pl.ANY)
    dma = pltpu.SemaphoreType.DMA
    return pl.pallas_call(
        out_kernel,
        in_specs=[anywhere, anywhere],
        out_specs=anywhere,
        out_shape=jax.ShapeDtypeStruct((rows, cols), BF16),
        scratch_shapes=[
            pltpu.VMEM((rows, channels), BF16),
            pltpu.VMEM((slots, channels, tile), BF16),
            pltpu.VMEM((slots, rows, tile), BF16),
            dma,
            dma((slots,)),
            dma((slots,)),
        ],
        compiler_params=pltpu.CompilerParams(vmem_limit_bytes=VMEM_BYTES),
        name="out_product",
    )(x2, dec_out)


def solution(mesh):
    head_split = P(None, "tp", None)
    whole_vec = P(None)
    whole_mat = P(None, None)
    in_specs = (P("dp", None, None), P("dp", "sp", None), whole_vec, head_split, head_split, head_split, P("tp", None, None), whole_vec, P(None, "tp"), P("tp", None), whole_vec, whole_vec, whole_mat, whole_mat, whole_mat, whole_mat, whole_vec, whole_mat, whole_mat, whole_mat)

    def local_step(latents, queries, lat_ln1, lat_wq, lat_wk, lat_wv, lat_wo, lat_ln2, lat_up, lat_down, dec_lnq, dec_lnkv, dec_wq, dec_wk, dec_wv, dec_wo, dec_ln, dec_up, dec_down, dec_out):
        lat_ws = [wt[:, 0, :].T for wt in (lat_wq, lat_wk, lat_wv)] + [lat_wo[0], lat_up.T, lat_down]
        gains = [lat_ln1, lat_ln2, dec_lnq, dec_lnkv, dec_ln]
        x2 = front(latents, queries, lat_ws, [dec_wq, dec_wk, dec_wv, dec_wo, dec_up, dec_down], gains)
        out = out_product(x2, dec_out)
        return out.reshape(queries.shape[0], queries.shape[1], dec_out.shape[1])

    return jax.shard_map(local_step, mesh=mesh, in_specs=in_specs, out_specs=P("dp", "sp", None), check_vma=False)
```

```python
import functools

import jax
import jax.numpy as jnp
from jax import lax
from jax.experimental import pallas as pl
from jax.experimental.pallas import tpu as pltpu
from jax.sharding import PartitionSpec as P

LN_EPS = 1e-5
MESH = pl.DeviceIdType.MESH
F32 = jnp.float32
BF16 = jnp.bfloat16
VMEM_BYTES = 67043328


def norm_rows(widened, gain_row):
    row_mean = jnp.mean(widened, axis=-1, keepdims=True)
    centred = widened - row_mean
    row_var = jnp.mean(jnp.square(centred), axis=-1, keepdims=True)
    return (centred * lax.rsqrt(row_var + LN_EPS) * gain_row).astype(BF16)


def gelu(val):
    return 0.5 * val * (1.0 + lax.erf(val * (0.5**0.5)))


def dot(lhs, rhs):
    return jnp.dot(lhs, rhs, preferred_element_type=F32)


def dot_t(lhs, rhs):
    return lax.dot_general(lhs, rhs, (((1,), (1,)), ((), ())), preferred_element_type=F32)


def softmax(scores):
    shifted = jnp.exp(scores - jnp.max(scores, axis=-1, keepdims=True))
    return (shifted / jnp.sum(shifted, axis=-1, keepdims=True)).astype(BF16)


def front_kernel(
    z_hbm, q_hbm, wq_hbm, wk_hbm, wv_hbm, wo_hbm, up_hbm, down_hbm, dwq_hbm, dwk_hbm, dwv_hbm, dwo_hbm, dup_hbm, ddn_hbm,
    g1_hbm, g2_hbm, gq_hbm, gkv_hbm, gd_hbm,
    x2_hbm,
    z, zr, wqkv, wo, wmlp, half, taken, queries, dwq, dwk, dwv, dwo, dup, ddn,
    g1, g2, gq, gkv, gd, normed, khead, vhead, part1, part2, kbuf, vbuf, qd, x2,
    load_sem, out_sem, pair_sem, x_sem, k1_sem, v1_sem, k2_sem, v2_sem, k3_sem, v3_sem, share_sem,
):
    sp, tp = lax.axis_index("sp"), lax.axis_index("tp")
    zc, yc = sp // 4, sp % 4
    xc, core = tp // 2, tp % 2
    items, latents, width = z.shape

    partner = {"tp": tp + 1 - 2 * core}
    x_peer = [{"tp": ((xc + d) % 4) * 2 + core} for d in (1, 2, 3)]
    y_peer = [{"sp": zc * 4 + (yc + d) % 4} for d in (1, 2, 3)]
    z_peer = [{"sp": ((zc + d) % 4) * 4 + yc} for d in (1, 2, 3)]

    def remote(src, dst, sems, where):
        copy = pltpu.make_async_remote_copy(
            src_ref=src, dst_ref=dst, send_sem=sems.at[0], recv_sem=sems.at[1], device_id=where, device_id_type=MESH)
        copy.start()
        return copy

    barrier = pltpu.get_barrier_semaphore()
    peers = [partner] + x_peer + y_peer + z_peer
    for peer in peers:
        pl.semaphore_signal(barrier, inc=1, device_id=peer, device_id_type=MESH)

    loads = []

    def load(src, dst):
        copy = pltpu.make_async_copy(src, dst, load_sem.at[len(loads)])
        copy.start()
        loads.append(copy)
        return copy

    load_g = [load(src, dst) for src, dst in ((g1_hbm, g1), (g2_hbm, g2), (gq_hbm, gq), (gkv_hbm, gkv), (gd_hbm, gd))]
    load_z = [load(z_hbm.at[0], z.at[0])]
    load_q = [load(src, wqkv.at[i]) for i, src in enumerate((wq_hbm, wk_hbm, wv_hbm))]
    load_z += [load(z_hbm.at[b], z.at[b]) for b in range(1, items)]
    load_zr = [load(z_hbm.at[:, pl.ds(pl.multiple_of(sp * 16 + at * 8, 8), 8), :], zr.at[i]) for i, at in enumerate((core, 1 - core))]
    load_r = [load(wo_hbm, wo), load(up_hbm, wmlp.at[0, 0]), load(down_hbm, wmlp.at[0, 1])]
    mine = latents // 2
    load_dq = [load(q_hbm.at[:, pl.ds(pl.multiple_of(core * mine, mine), mine), :], queries), load(dwq_hbm, dwq)]
    load_kv = [load(dwk_hbm, dwk), load(dwv_hbm, dwv)]
    load_dec = [load(dwo_hbm, dwo), load(dup_hbm, dup), load(ddn_hbm, ddn)]

    def norm_item(b):
        for at in range(0, latents, 32):
            normed[b * latents + at : b * latents + at + 32, :] = norm_rows(z[b, at : at + 32, :].astype(F32), g1[...])

    def item(ref, b):
        return ref[latents * b : latents * (b + 1), :]

    def project(b):
        khead[latents * b : latents * (b + 1), :] = dot_t(item(normed, b), wqkv[1]).astype(BF16)
        vhead[latents * b : latents * (b + 1), :] = dot_t(item(normed, b), wqkv[2]).astype(BF16)

    def attend(b):
        chip_rows = jnp.concatenate([zr[0, b].astype(F32), zr[1, b].astype(F32)], axis=0)
        q_rows = dot_t(norm_rows(chip_rows, g1[...]), wqkv[0]).astype(BF16)
        probs = softmax(dot_t(q_rows, item(khead, b)) * q_rows.shape[1] ** -0.5)
        context = dot(probs, item(vhead, b)).astype(BF16)
        return dot(context, wo[...])

    pair, sent1 = [], []

    def give(b, part):
        half[b] = part[8:].astype(BF16)
        pair.append(remote(half.at[b], taken.at[b], pair_sem.at[b], partner))

    def spread(b, part):
        pair[b].wait_recv()
        part1[b, xc] = (part[:8] + taken[b].astype(F32)).astype(BF16)
        sent1.append([remote(part1.at[b, xc], part1.at[b, xc], x_sem.at[0, b, d], x_peer[d]) for d in range(3)])

    for copy in load_g + load_z[:1]:
        copy.wait()
    norm_item(0)
    for copy in load_q + load_z[1:] + load_zr + load_r[:1]:
        copy.wait()
    project(0)
    norm_item(1)
    parts = [attend(0)]
    project(1)
    norm_item(2)
    pl.semaphore_wait(barrier, len(peers))
    give(0, parts[0])
    parts.append(attend(1))
    project(2)
    give(1, parts[1])
    parts.append(attend(2))
    spread(0, parts[0])
    give(2, parts[2])
    for copy in load_r[1:]:
        copy.wait()
    swap_r = remote(wmlp.at[0], wmlp.at[1], pair_sem.at[items], partner)
    spread(1, parts[1])
    spread(2, parts[2])

    for copy in load_dq:
        copy.wait()
    for b in range(items):
        qd[b] = dot(norm_rows(queries[b].astype(F32), gq[...]), dwq[...]).astype(BF16)

    def gather_sum(part, b):
        total = part[b, 0].astype(F32)
        for s in range(1, 4):
            total = total + part[b, s].astype(F32)
        return total

    sent2, z_mid = [], []
    for b in range(items):
        for copy in sent1[b]:
            copy.wait_recv()
        if b == 0:
            swap_r.wait_recv()
        z_mid.append((zr[0, b].astype(F32) + gather_sum(part1, b)).astype(BF16))
        normed_mid = norm_rows(z_mid[b].astype(F32), g2[...])
        mlp = jnp.zeros((8, width), F32)
        for h in range(2):
            hidden = gelu(dot_t(normed_mid, wmlp[h, 0])).astype(BF16)
            mlp = mlp + dot(hidden, wmlp[h, 1])
        part2[b, xc] = mlp.astype(BF16)
        sent2.append([remote(part2.at[b, xc], part2.at[b, xc], x_sem.at[1, b, d], x_peer[d]) for d in range(3)])

    for copy in load_kv:
        copy.wait()
    k1, v1 = [], []
    for b in range(items):
        for copy in sent2[b]:
            copy.wait_recv()
        z_new = (z_mid[b].astype(F32) + gather_sum(part2, b)).astype(BF16)
        kv_in = norm_rows(z_new.astype(F32), gkv[...])
        kbuf[b, core, zc, yc] = dot(kv_in, dwk[...]).astype(BF16)
        vbuf[b, core, zc, yc] = dot(kv_in, dwv[...]).astype(BF16)
        k1.append([remote(kbuf.at[b, core, zc, yc], kbuf.at[b, core, zc, yc], k1_sem.at[b, d], y_peer[d]) for d in range(3)])
        v1.append([remote(vbuf.at[b, core, zc, yc], vbuf.at[b, core, zc, yc], v1_sem.at[b, d], z_peer[d]) for d in range(3)])

    for copy in load_dec:
        copy.wait()
    k2, v2, k3, v3 = [], [], [], []

    def forward_k(b, at, i):
        k3[b].append(remote(kbuf.at[b, core, at], kbuf.at[b, core, at], k3_sem.at[b, i], partner))

    def forward_v(b, at, i):
        v3[b].append(remote(vbuf.at[b, core, :, at], vbuf.at[b, core, :, at], v3_sem.at[b, i], partner))

    for b in range(items):
        k3.append([])
        v3.append([])
        for copy in k1[b]:
            copy.wait_recv()
        k2.append([remote(kbuf.at[b, core, zc], kbuf.at[b, core, zc], k2_sem.at[b, d], z_peer[d]) for d in range(3)])
        for copy in v1[b]:
            copy.wait_recv()
        v2.append([remote(vbuf.at[b, core, :, yc], vbuf.at[b, core, :, yc], v2_sem.at[b, d], y_peer[d]) for d in range(3)])
        forward_k(b, zc, 3)
        forward_v(b, yc, 3)

    def swap(b):
        for d in (0, 2, 1):
            k2[b][d].wait_recv()
            forward_k(b, (zc + 3 - d) % 4, d)
            v2[b][d].wait_recv()
            forward_v(b, (yc + 3 - d) % 4, d)

    stores, mixes, shared = [], [], []
    channels = qd.shape[2]

    def decode_first(b):
        q_item = qd[b]
        for copy in k3[b]:
            copy.wait_recv()
        keys = kbuf[b].astype(F32).reshape(latents, channels).astype(BF16)
        probs = softmax(dot_t(q_item, keys) * channels**-0.5)
        for copy in v3[b]:
            copy.wait_recv()
        values = vbuf[b].astype(F32).reshape(latents, channels).astype(BF16)
        context = dot(probs, values).astype(BF16)
        mixes.append((q_item.astype(F32) + dot(context, dwo[...])).astype(BF16))

    def decode_last(b):
        mixed = mixes[b]
        hidden = gelu(dot(norm_rows(mixed.astype(F32), gd[...]), dup[...])).astype(BF16)
        x2[b] = (mixed.astype(F32) + dot(hidden, ddn[...])).astype(BF16)
        dst = x2_hbm.at[pl.ds(pl.multiple_of(latents * b + core * mine, mine), mine)]
        shared.append(remote(x2.at[b], dst, share_sem.at[b], partner))
        store = pltpu.make_async_copy(x2.at[b], dst, out_sem.at[b])
        store.start()
        stores.append(store)

    swap(0)
    for b in range(items):
        decode_first(b)
        if b + 1 < items:
            swap(b + 1)
        decode_last(b)

    for copy in shared:
        copy.wait_recv()
    for copy in shared + pair + [swap_r] + sum(sent1 + sent2 + k1 + v1 + k2 + v2 + k3 + v3, []):
        copy.wait_send()
    for store in stores:
        store.wait()


def front(latents, queries, lat_ws, dec_ws, gains):
    items, lat_rows, width = latents.shape
    channels = queries.shape[2]
    head = lat_ws[0].shape[0]
    anywhere = pl.BlockSpec(memory_space=pl.ANY)
    total = items * lat_rows
    dma = pltpu.SemaphoreType.DMA
    return pl.pallas_call(
        front_kernel,
        out_shape=jax.ShapeDtypeStruct((total, channels), BF16),
        in_specs=[anywhere] * 19,
        out_specs=anywhere,
        scratch_shapes=[
            pltpu.VMEM((items, lat_rows, width), BF16),
            pltpu.VMEM((2, items, 8, width), BF16),
            pltpu.VMEM((3, head, width), BF16),
            pltpu.VMEM((head, width), BF16),
            pltpu.VMEM((2, 2, head, width), BF16),
            pltpu.VMEM((items, 8, width), BF16),
            pltpu.VMEM((items, 8, width), BF16),
            pltpu.VMEM((items, lat_rows // 2, channels), BF16),
            pltpu.VMEM((channels, channels), BF16),
            pltpu.VMEM((width, channels), BF16),
            pltpu.VMEM((width, channels), BF16),
            pltpu.VMEM((channels, channels), BF16),
            pltpu.VMEM((channels, channels), BF16),
            pltpu.VMEM((channels, channels), BF16),
            pltpu.VMEM((width,), F32),
            pltpu.VMEM((width,), F32),
            pltpu.VMEM((channels,), F32),
            pltpu.VMEM((width,), F32),
            pltpu.VMEM((channels,), F32),
            pltpu.VMEM((total, width), BF16),
            pltpu.VMEM((total, head), BF16),
            pltpu.VMEM((total, head), BF16),
            pltpu.VMEM((items, 4, 8, width), BF16),
            pltpu.VMEM((items, 4, 8, width), BF16),
            pltpu.VMEM((items, 2, 4, 4, 8, channels), BF16),
            pltpu.VMEM((items, 2, 4, 4, 8, channels), BF16),
            pltpu.VMEM((items, lat_rows // 2, channels), BF16),
            pltpu.VMEM((items, lat_rows // 2, channels), BF16),
            dma((23,)),
            dma((items,)),
            dma((items + 1, 2)),
            dma((2, items, 3, 2)),
            dma((items, 3, 2)),
            dma((items, 3, 2)),
            dma((items, 3, 2)),
            dma((items, 3, 2)),
            dma((items, 4, 2)),
            dma((items, 4, 2)),
            dma((items, 2)),
        ],
        compiler_params=pltpu.CompilerParams(collective_id=0, has_side_effects=True, vmem_limit_bytes=VMEM_BYTES),
        name="front",
    )(latents, queries, *lat_ws, *dec_ws, *gains)


def out_kernel(plan, x2_hbm, wt_hbm, out_hbm, x2, wt, out, x2_sem, wt_sem, out_sem):
    head, (reps, tile), tail = plan
    starts = [sum(head[:t]) for t in range(len(head))]
    base = sum(head)
    ends = [base + reps * tile + sum(tail[:t]) for t in range(len(tail))]
    fixed = list(zip(starts, head)), list(zip(ends, tail))
    steps = len(head) + reps + len(tail)

    def place(i):
        if isinstance(i, int):
            if i < len(head):
                return fixed[0][i]
            if i >= len(head) + reps:
                return fixed[1][i - len(head) - reps]
        return base + (i - len(head)) * tile, tile

    def fetch(i):
        at, width = place(i)
        at = pl.multiple_of(at, 128)
        return pltpu.make_async_copy(wt_hbm.at[:, pl.ds(at, width)], wt.at[i % 2, :, :width], wt_sem.at[i % 2])

    def store(i):
        at, width = place(i)
        at = pl.multiple_of(at, 128)
        return pltpu.make_async_copy(out.at[i % 2, :, :width], out_hbm.at[:, pl.ds(at, width)], out_sem.at[i % 2])

    def product(i):
        width = place(i)[1]
        for at in range(0, x2.shape[0], 384):
            out[i % 2, at : at + 384, :width] = dot(x2[at : at + 384, :], wt[i % 2, :, :width]).astype(BF16)

    def one(i):
        if i + 1 < steps:
            fetch(i + 1).start()
        fetch(i).wait()
        if i >= 2:
            store(i - 2).wait()
        product(i)
        store(i).start()

    load_x2 = pltpu.make_async_copy(x2_hbm, x2, x2_sem)
    load_x2.start()
    fetch(0).start()
    load_x2.wait()
    for i in range(len(head)):
        one(i)
    lo, hi = len(head), len(head) + reps

    def step(i, carry):
        @pl.when(i + 1 < hi)
        def _():
            fetch(i + 1).start()

        @pl.when(i + 1 == hi)
        def _():
            fetch(hi).start()

        fetch(i).wait()
        for t in (lo, lo + 1):
            @pl.when(i == t)
            def _(t=t):
                store(t - 2).wait()

        @pl.when(i >= lo + 2)
        def _():
            store(i - 2).wait()

        product(i)
        store(i).start()
        return carry

    lax.fori_loop(lo, hi, step, 0)
    for i in range(hi, steps):
        one(i)
    store(steps - 2).wait()
    store(steps - 1).wait()


def out_product(x2, dec_out):
    rows, channels = x2.shape
    cols = dec_out.shape[1]
    tile = 4096
    head, tail = (1280, 3072), (2048, 1024)
    plan = (head, ((cols - sum(head) - sum(tail)) // tile, tile), tail)
    anywhere = pl.BlockSpec(memory_space=pl.ANY)
    dma = pltpu.SemaphoreType.DMA
    return pl.pallas_call(
        functools.partial(out_kernel, plan),
        in_specs=[anywhere, anywhere],
        out_specs=anywhere,
        out_shape=jax.ShapeDtypeStruct((rows, cols), BF16),
        scratch_shapes=[
            pltpu.VMEM((rows, channels), BF16),
            pltpu.VMEM((2, channels, tile), BF16),
            pltpu.VMEM((2, rows, tile), BF16),
            dma,
            dma((2,)),
            dma((2,)),
        ],
        compiler_params=pltpu.CompilerParams(vmem_limit_bytes=VMEM_BYTES),
        name="out_product",
    )(x2, dec_out)


def solution(mesh):
    head_split = P(None, "tp", None)
    whole_vec = P(None)
    whole_mat = P(None, None)
    in_specs = (P("dp", None, None), P("dp", "sp", None), whole_vec, head_split, head_split, head_split, P("tp", None, None), whole_vec, P(None, "tp"), P("tp", None), whole_vec, whole_vec, whole_mat, whole_mat, whole_mat, whole_mat, whole_vec, whole_mat, whole_mat, whole_mat)

    def local_step(latents, queries, lat_ln1, lat_wq, lat_wk, lat_wv, lat_wo, lat_ln2, lat_up, lat_down, dec_lnq, dec_lnkv, dec_wq, dec_wk, dec_wv, dec_wo, dec_ln, dec_up, dec_down, dec_out):
        lat_ws = [wt[:, 0, :].T for wt in (lat_wq, lat_wk, lat_wv)] + [lat_wo[0], lat_up.T, lat_down]
        gains = [lat_ln1, lat_ln2, dec_lnq, dec_lnkv, dec_ln]
        x2 = front(latents, queries, lat_ws, [dec_wq, dec_wk, dec_wv, dec_wo, dec_up, dec_down], gains)
        out = out_product(x2, dec_out)
        return out.reshape(queries.shape[0], queries.shape[1], dec_out.shape[1])

    return jax.shard_map(local_step, mesh=mesh, in_specs=in_specs, out_specs=P("dp", "sp", None), check_vma=False)
```

```python
import functools

import jax
import jax.numpy as jnp
from jax import lax
from jax.experimental import pallas as pl
from jax.experimental.pallas import tpu as pltpu
from jax.sharding import PartitionSpec as P

LN_EPS = 1e-5
MESH = pl.DeviceIdType.MESH
F32 = jnp.float32
BF16 = jnp.bfloat16
VMEM_BYTES = 67043328
FIRST_COLS = 2048
HANDED = 4600 * 1024


def norm_rows(widened, gain_row):
    row_mean = jnp.mean(widened, axis=-1, keepdims=True)
    centred = widened - row_mean
    row_var = jnp.mean(jnp.square(centred), axis=-1, keepdims=True)
    return (centred * lax.rsqrt(row_var + LN_EPS) * gain_row).astype(BF16)


def gelu(val):
    return 0.5 * val * (1.0 + lax.erf(val * (0.5**0.5)))


def dot(lhs, rhs):
    return jnp.dot(lhs, rhs, preferred_element_type=F32)


def dot_t(lhs, rhs):
    return lax.dot_general(lhs, rhs, (((1,), (1,)), ((), ())), preferred_element_type=F32)


def softmax(scores):
    shifted = jnp.exp(scores - jnp.max(scores, axis=-1, keepdims=True))
    return (shifted / jnp.sum(shifted, axis=-1, keepdims=True)).astype(BF16)


def front_kernel(
    z_hbm, q_hbm, wq_hbm, wk_hbm, wv_hbm, wo_hbm, up_hbm, down_hbm, dwq_hbm, dwk_hbm, dwv_hbm, dwo_hbm, dup_hbm, ddn_hbm,
    g1_hbm, g2_hbm, gq_hbm, gkv_hbm, gd_hbm, wout_hbm,
    x2, first,
    z, zr, wqkv, wo, wmlp, half, taken, queries, dwq, dwk, dwv, dwo, dup, ddn,
    g1, g2, gq, gkv, gd, normed, khead, vhead, part1, part2, kbuf, vbuf, qd,
    load_sem, pair_sem, x_sem, k1_sem, v1_sem, k2_sem, v2_sem, k3_sem, v3_sem, share_sem,
):
    sp, tp = lax.axis_index("sp"), lax.axis_index("tp")
    zc, yc = sp // 4, sp % 4
    xc, core = tp // 2, tp % 2
    items, latents, width = z.shape

    partner = {"tp": tp + 1 - 2 * core}
    x_peer = [{"tp": ((xc + d) % 4) * 2 + core} for d in (1, 2, 3)]
    y_peer = [{"sp": zc * 4 + (yc + d) % 4} for d in (1, 2, 3)]
    z_peer = [{"sp": ((zc + d) % 4) * 4 + yc} for d in (1, 2, 3)]

    def remote(src, dst, sems, where):
        copy = pltpu.make_async_remote_copy(
            src_ref=src, dst_ref=dst, send_sem=sems.at[0], recv_sem=sems.at[1], device_id=where, device_id_type=MESH)
        copy.start()
        return copy

    barrier = pltpu.get_barrier_semaphore()
    peers = [partner] + x_peer + y_peer + z_peer
    for peer in peers:
        pl.semaphore_signal(barrier, inc=1, device_id=peer, device_id_type=MESH)

    loads = []

    def load(src, dst):
        copy = pltpu.make_async_copy(src, dst, load_sem.at[len(loads)])
        copy.start()
        loads.append(copy)
        return copy

    load_g = [load(src, dst) for src, dst in ((g1_hbm, g1), (g2_hbm, g2), (gq_hbm, gq), (gkv_hbm, gkv), (gd_hbm, gd))]
    load_z = [load(z_hbm.at[0], z.at[0])]
    load_q = [load(src, wqkv.at[i]) for i, src in enumerate((wq_hbm, wk_hbm, wv_hbm))]
    load_z += [load(z_hbm.at[b], z.at[b]) for b in range(1, items)]
    load_zr = [load(z_hbm.at[:, pl.ds(pl.multiple_of(sp * 16 + at * 8, 8), 8), :], zr.at[i]) for i, at in enumerate((core, 1 - core))]
    load_r = [load(wo_hbm, wo), load(up_hbm, wmlp.at[0, 0]), load(down_hbm, wmlp.at[0, 1])]
    mine = latents // 2

    def norm_item(b):
        for at in range(0, latents, 32):
            normed[b * latents + at : b * latents + at + 32, :] = norm_rows(z[b, at : at + 32, :].astype(F32), g1[...])

    def item(ref, b):
        return ref[latents * b : latents * (b + 1), :]

    def project(b):
        khead[latents * b : latents * (b + 1), :] = dot_t(item(normed, b), wqkv[1]).astype(BF16)
        vhead[latents * b : latents * (b + 1), :] = dot_t(item(normed, b), wqkv[2]).astype(BF16)

    def attend(b):
        chip_rows = jnp.concatenate([zr[0, b].astype(F32), zr[1, b].astype(F32)], axis=0)
        q_rows = dot_t(norm_rows(chip_rows, g1[...]), wqkv[0]).astype(BF16)
        probs = softmax(dot_t(q_rows, item(khead, b)) * q_rows.shape[1] ** -0.5)
        context = dot(probs, item(vhead, b)).astype(BF16)
        return dot(context, wo[...])

    pair, sent1 = [], []

    def give(b, part):
        half[b] = part[8:].astype(BF16)
        pair.append(remote(half.at[b], taken.at[b], pair_sem.at[b], partner))

    def spread(b, part):
        pair[b].wait_recv()
        part1[b, xc] = (part[:8] + taken[b].astype(F32)).astype(BF16)
        sent1.append([remote(part1.at[b, xc], part1.at[b, xc], x_sem.at[0, b, d], x_peer[d]) for d in range(3)])

    for copy in load_g + load_z[:1]:
        copy.wait()
    norm_item(0)
    for copy in load_q + load_z[1:] + load_zr + load_r[:1]:
        copy.wait()
    load_dq = [load(q_hbm.at[:, pl.ds(pl.multiple_of(core * mine, mine), mine), :], queries), load(dwq_hbm, dwq)]
    load_kv = [load(dwk_hbm, dwk), load(dwv_hbm, dwv)]
    load_dec = [load(dwo_hbm, dwo), load(dup_hbm, dup), load(ddn_hbm, ddn)]
    load_first = load(wout_hbm.at[:, : first.shape[1]], first)
    project(0)
    norm_item(1)
    parts = [attend(0)]
    project(1)
    norm_item(2)
    pl.semaphore_wait(barrier, len(peers))
    give(0, parts[0])
    parts.append(attend(1))
    project(2)
    give(1, parts[1])
    parts.append(attend(2))
    spread(0, parts[0])
    give(2, parts[2])
    for copy in load_r[1:]:
        copy.wait()
    swap_r = remote(wmlp.at[0], wmlp.at[1], pair_sem.at[items], partner)
    spread(1, parts[1])
    spread(2, parts[2])

    for copy in load_dq:
        copy.wait()
    for b in range(items):
        qd[b] = dot(norm_rows(queries[b].astype(F32), gq[...]), dwq[...]).astype(BF16)

    def gather_sum(part, b):
        total = part[b, 0].astype(F32)
        for s in range(1, 4):
            total = total + part[b, s].astype(F32)
        return total

    sent2, z_mid = [], []
    for b in range(items):
        for copy in sent1[b]:
            copy.wait_recv()
        if b == 0:
            swap_r.wait_recv()
        z_mid.append((zr[0, b].astype(F32) + gather_sum(part1, b)).astype(BF16))
        normed_mid = norm_rows(z_mid[b].astype(F32), g2[...])
        mlp = jnp.zeros((8, width), F32)
        for h in range(2):
            hidden = gelu(dot_t(normed_mid, wmlp[h, 0])).astype(BF16)
            mlp = mlp + dot(hidden, wmlp[h, 1])
        part2[b, xc] = mlp.astype(BF16)
        sent2.append([remote(part2.at[b, xc], part2.at[b, xc], x_sem.at[1, b, d], x_peer[d]) for d in range(3)])

    for copy in load_kv:
        copy.wait()
    k1, v1 = [], []
    for b in range(items):
        for copy in sent2[b]:
            copy.wait_recv()
        z_new = (z_mid[b].astype(F32) + gather_sum(part2, b)).astype(BF16)
        kv_in = norm_rows(z_new.astype(F32), gkv[...])
        kbuf[b, core, zc, yc] = dot(kv_in, dwk[...]).astype(BF16)
        vbuf[b, core, zc, yc] = dot(kv_in, dwv[...]).astype(BF16)
        k1.append([remote(kbuf.at[b, core, zc, yc], kbuf.at[b, core, zc, yc], k1_sem.at[b, d], y_peer[d]) for d in range(3)])
        v1.append([remote(vbuf.at[b, core, zc, yc], vbuf.at[b, core, zc, yc], v1_sem.at[b, d], z_peer[d]) for d in range(3)])

    for copy in load_dec:
        copy.wait()
    k2, v2, k3, v3 = [], [], [], []

    def forward_k(b, at, i):
        k3[b].append(remote(kbuf.at[b, core, at], kbuf.at[b, core, at], k3_sem.at[b, i], partner))

    def forward_v(b, at, i):
        v3[b].append(remote(vbuf.at[b, core, :, at], vbuf.at[b, core, :, at], v3_sem.at[b, i], partner))

    for b in range(items):
        k3.append([])
        v3.append([])
        for copy in k1[b]:
            copy.wait_recv()
        k2.append([remote(kbuf.at[b, core, zc], kbuf.at[b, core, zc], k2_sem.at[b, d], z_peer[d]) for d in range(3)])
        for copy in v1[b]:
            copy.wait_recv()
        v2.append([remote(vbuf.at[b, core, :, yc], vbuf.at[b, core, :, yc], v2_sem.at[b, d], y_peer[d]) for d in range(3)])
        forward_k(b, zc, 3)
        forward_v(b, yc, 3)

    def swap(b):
        for d in (0, 2, 1):
            k2[b][d].wait_recv()
            forward_k(b, (zc + 3 - d) % 4, d)
            v2[b][d].wait_recv()
            forward_v(b, (yc + 3 - d) % 4, d)

    mixes, shared = [], []
    channels = qd.shape[2]

    def decode_first(b):
        q_item = qd[b]
        for copy in k3[b]:
            copy.wait_recv()
        keys = kbuf[b].astype(F32).reshape(latents, channels).astype(BF16)
        probs = softmax(dot_t(q_item, keys) * channels**-0.5)
        for copy in v3[b]:
            copy.wait_recv()
        values = vbuf[b].astype(F32).reshape(latents, channels).astype(BF16)
        context = dot(probs, values).astype(BF16)
        mixes.append((q_item.astype(F32) + dot(context, dwo[...])).astype(BF16))

    def decode_last(b):
        mixed = mixes[b]
        hidden = gelu(dot(norm_rows(mixed.astype(F32), gd[...]), dup[...])).astype(BF16)
        rows = pl.ds(pl.multiple_of(latents * b + core * mine, mine), mine)
        x2[rows, :] = (mixed.astype(F32) + dot(hidden, ddn[...])).astype(BF16)
        shared.append(remote(x2.at[rows], x2.at[rows], share_sem.at[b], partner))

    swap(0)
    for b in range(items):
        decode_first(b)
        if b + 1 < items:
            swap(b + 1)
        decode_last(b)

    for copy in shared:
        copy.wait_recv()
    for copy in shared + pair + [swap_r] + sum(sent1 + sent2 + k1 + v1 + k2 + v2 + k3 + v3, []):
        copy.wait_send()
    load_first.wait()


def front(latents, queries, lat_ws, dec_ws, gains, dec_out):
    items, lat_rows, width = latents.shape
    channels = queries.shape[2]
    head = lat_ws[0].shape[0]
    anywhere = pl.BlockSpec(memory_space=pl.ANY)
    total = items * lat_rows
    dma = pltpu.SemaphoreType.DMA
    return pl.pallas_call(
        front_kernel,
        out_shape=[pltpu.VMEM((total, channels), BF16), pltpu.VMEM((channels, FIRST_COLS), BF16)],
        in_specs=[anywhere] * 20,
        out_specs=[pl.BlockSpec(memory_space=pltpu.VMEM)] * 2,
        scratch_shapes=[
            pltpu.VMEM((items, lat_rows, width), BF16),
            pltpu.VMEM((2, items, 8, width), BF16),
            pltpu.VMEM((3, head, width), BF16),
            pltpu.VMEM((head, width), BF16),
            pltpu.VMEM((2, 2, head, width), BF16),
            pltpu.VMEM((items, 8, width), BF16),
            pltpu.VMEM((items, 8, width), BF16),
            pltpu.VMEM((items, lat_rows // 2, channels), BF16),
            pltpu.VMEM((channels, channels), BF16),
            pltpu.VMEM((width, channels), BF16),
            pltpu.VMEM((width, channels), BF16),
            pltpu.VMEM((channels, channels), BF16),
            pltpu.VMEM((channels, channels), BF16),
            pltpu.VMEM((channels, channels), BF16),
            pltpu.VMEM((width,), F32),
            pltpu.VMEM((width,), F32),
            pltpu.VMEM((channels,), F32),
            pltpu.VMEM((width,), F32),
            pltpu.VMEM((channels,), F32),
            pltpu.VMEM((total, width), BF16),
            pltpu.VMEM((total, head), BF16),
            pltpu.VMEM((total, head), BF16),
            pltpu.VMEM((items, 4, 8, width), BF16),
            pltpu.VMEM((items, 4, 8, width), BF16),
            pltpu.VMEM((items, 2, 4, 4, 8, channels), BF16),
            pltpu.VMEM((items, 2, 4, 4, 8, channels), BF16),
            pltpu.VMEM((items, lat_rows // 2, channels), BF16),
            dma((24,)),
            dma((items + 1, 2)),
            dma((2, items, 3, 2)),
            dma((items, 3, 2)),
            dma((items, 3, 2)),
            dma((items, 3, 2)),
            dma((items, 3, 2)),
            dma((items, 4, 2)),
            dma((items, 4, 2)),
            dma((items, 2)),
        ],
        compiler_params=pltpu.CompilerParams(collective_id=0, has_side_effects=True, vmem_limit_bytes=VMEM_BYTES - HANDED),
        name="front",
    )(latents, queries, *lat_ws, *dec_ws, *gains, dec_out)


def out_kernel(plan, x2, first, wt_hbm, out_hbm, wt, out, wt_sem, out_sem):
    head, (reps, tile), tail = plan
    starts = [sum(head[:t]) for t in range(len(head))]
    base = sum(head)
    ends = [base + reps * tile + sum(tail[:t]) for t in range(len(tail))]
    fixed = list(zip(starts, head)), list(zip(ends, tail))
    steps = len(head) + reps + len(tail)

    def place(i):
        if isinstance(i, int):
            if i < len(head):
                return fixed[0][i]
            if i >= len(head) + reps:
                return fixed[1][i - len(head) - reps]
        return base + (i - len(head)) * tile, tile

    def fetch(i):
        at, width = place(i)
        at = pl.multiple_of(at, 128)
        return pltpu.make_async_copy(wt_hbm.at[:, pl.ds(at, width)], wt.at[i % 2, :, :width], wt_sem.at[i % 2])

    def store(i):
        at, width = place(i)
        at = pl.multiple_of(at, 128)
        return pltpu.make_async_copy(out.at[i % 2, :, :width], out_hbm.at[:, pl.ds(at, width)], out_sem.at[i % 2])

    def product(i):
        width = place(i)[1]
        for at in range(0, x2.shape[0], 384):
            weights = first[...] if isinstance(i, int) and i == 0 else wt[i % 2, :, :width]
            out[i % 2, at : at + 384, :width] = dot(x2[at : at + 384, :], weights).astype(BF16)

    def one(i):
        if i + 1 < steps:
            fetch(i + 1).start()
        if i:
            fetch(i).wait()
        if i >= 2:
            store(i - 2).wait()
        product(i)
        store(i).start()

    for i in range(len(head)):
        one(i)
    lo, hi = len(head), len(head) + reps

    def step(i, carry):
        @pl.when(i + 1 < hi)
        def _():
            fetch(i + 1).start()

        @pl.when(i + 1 == hi)
        def _():
            fetch(hi).start()

        fetch(i).wait()
        for t in (lo, lo + 1):
            @pl.when(i == t)
            def _(t=t):
                store(t - 2).wait()

        @pl.when(i >= lo + 2)
        def _():
            store(i - 2).wait()

        product(i)
        store(i).start()
        return carry

    lax.fori_loop(lo, hi, step, 0)
    for i in range(hi, steps):
        one(i)
    store(steps - 2).wait()
    store(steps - 1).wait()


def out_product(x2, first, dec_out):
    rows, channels = x2.shape
    cols = dec_out.shape[1]
    tile = 4096
    head, tail = (FIRST_COLS, 3072), (1280, 1024)
    plan = (head, ((cols - sum(head) - sum(tail)) // tile, tile), tail)
    anywhere = pl.BlockSpec(memory_space=pl.ANY)
    dma = pltpu.SemaphoreType.DMA
    return pl.pallas_call(
        functools.partial(out_kernel, plan),
        in_specs=[pl.BlockSpec(memory_space=pltpu.VMEM)] * 2 + [anywhere],
        out_specs=anywhere,
        out_shape=jax.ShapeDtypeStruct((rows, cols), BF16),
        scratch_shapes=[
            pltpu.VMEM((2, channels, tile), BF16),
            pltpu.VMEM((2, rows, tile), BF16),
            dma((2,)),
            dma((2,)),
        ],
        compiler_params=pltpu.CompilerParams(vmem_limit_bytes=40 * 2**20),
        name="out_product",
    )(x2, first, dec_out)


def solution(mesh):
    head_split = P(None, "tp", None)
    whole_vec = P(None)
    whole_mat = P(None, None)
    in_specs = (P("dp", None, None), P("dp", "sp", None), whole_vec, head_split, head_split, head_split, P("tp", None, None), whole_vec, P(None, "tp"), P("tp", None), whole_vec, whole_vec, whole_mat, whole_mat, whole_mat, whole_mat, whole_vec, whole_mat, whole_mat, whole_mat)

    def local_step(latents, queries, lat_ln1, lat_wq, lat_wk, lat_wv, lat_wo, lat_ln2, lat_up, lat_down, dec_lnq, dec_lnkv, dec_wq, dec_wk, dec_wv, dec_wo, dec_ln, dec_up, dec_down, dec_out):
        lat_ws = [wt[:, 0, :].T for wt in (lat_wq, lat_wk, lat_wv)] + [lat_wo[0], lat_up.T, lat_down]
        gains = [lat_ln1, lat_ln2, dec_lnq, dec_lnkv, dec_ln]
        x2, first = front(latents, queries, lat_ws, [dec_wq, dec_wk, dec_wv, dec_wo, dec_up, dec_down], gains, dec_out)
        out = out_product(x2, first, dec_out)
        return out.reshape(queries.shape[0], queries.shape[1], dec_out.shape[1])

    return jax.shard_map(local_step, mesh=mesh, in_specs=in_specs, out_specs=P("dp", "sp", None), check_vma=False)
```

```python
import functools

import jax
import jax.numpy as jnp
from jax import lax
from jax.experimental import pallas as pl
from jax.experimental.pallas import tpu as pltpu
from jax.sharding import PartitionSpec as P

LN_EPS = 1e-5
MESH = pl.DeviceIdType.MESH
F32 = jnp.float32
BF16 = jnp.bfloat16
VMEM_BYTES = 67043328
FIRST_COLS = 2048
HANDED = 4600 * 1024


def norm_rows(widened, gain_row):
    row_mean = jnp.mean(widened, axis=-1, keepdims=True)
    centred = widened - row_mean
    row_var = jnp.mean(jnp.square(centred), axis=-1, keepdims=True)
    return (centred * lax.rsqrt(row_var + LN_EPS) * gain_row).astype(BF16)


def gelu(val):
    return 0.5 * val * (1.0 + lax.erf(val * (0.5**0.5)))


def dot(lhs, rhs):
    return jnp.dot(lhs, rhs, preferred_element_type=F32)


def dot_t(lhs, rhs):
    return lax.dot_general(lhs, rhs, (((1,), (1,)), ((), ())), preferred_element_type=F32)


def softmax(scores):
    shifted = jnp.exp(scores - jnp.max(scores, axis=-1, keepdims=True))
    return (shifted / jnp.sum(shifted, axis=-1, keepdims=True)).astype(BF16)


def front_kernel(
    z_hbm, q_hbm, wq_hbm, wk_hbm, wv_hbm, wo_hbm, up_hbm, down_hbm, dwq_hbm, dwk_hbm, dwv_hbm, dwo_hbm, dup_hbm, ddn_hbm,
    g1_hbm, g2_hbm, gq_hbm, gkv_hbm, gd_hbm, wout_hbm,
    x2, first,
    z, zr, wqkv, wo, wmlp, half, taken, queries, dwq, dwkv, dwo, dup, ddn,
    g1, g2, gq, gkv, gd, normed, khead, vhead, part1, part2, kbuf, vbuf, qd,
    load_sem, pair_sem, x_sem, k1_sem, v1_sem, k2_sem, v2_sem, k3_sem, v3_sem, share_sem,
):
    sp, tp = lax.axis_index("sp"), lax.axis_index("tp")
    zc, yc = sp // 4, sp % 4
    xc, core = tp // 2, tp % 2
    items, latents, width = z.shape

    partner = {"tp": tp + 1 - 2 * core}
    x_peer = [{"tp": ((xc + d) % 4) * 2 + core} for d in (1, 2, 3)]
    y_peer = [{"sp": zc * 4 + (yc + d) % 4} for d in (1, 2, 3)]
    z_peer = [{"sp": ((zc + d) % 4) * 4 + yc} for d in (1, 2, 3)]

    def remote(src, dst, sems, where):
        copy = pltpu.make_async_remote_copy(
            src_ref=src, dst_ref=dst, send_sem=sems.at[0], recv_sem=sems.at[1], device_id=where, device_id_type=MESH)
        copy.start()
        return copy

    barrier = pltpu.get_barrier_semaphore()
    peers = [partner] + x_peer + y_peer + z_peer
    for peer in peers:
        pl.semaphore_signal(barrier, inc=1, device_id=peer, device_id_type=MESH)

    loads = []

    def load(src, dst):
        copy = pltpu.make_async_copy(src, dst, load_sem.at[len(loads)])
        copy.start()
        loads.append(copy)
        return copy

    load_g = [load(src, dst) for src, dst in ((g1_hbm, g1), (g2_hbm, g2), (gq_hbm, gq), (gkv_hbm, gkv), (gd_hbm, gd))]
    load_z = [load(z_hbm.at[0], z.at[0])]
    load_q = [load(src, wqkv.at[i]) for i, src in enumerate((wq_hbm, wk_hbm, wv_hbm))]
    load_z += [load(z_hbm.at[b], z.at[b]) for b in range(1, items)]
    load_zr = [load(z_hbm.at[:, pl.ds(pl.multiple_of(sp * 16 + at * 8, 8), 8), :], zr.at[i]) for i, at in enumerate((core, 1 - core))]
    load_r = [load(wo_hbm, wo), load(up_hbm, wmlp.at[0, 0]), load(down_hbm, wmlp.at[0, 1])]
    mine = latents // 2

    def norm_item(b):
        for at in range(0, latents, 32):
            normed[b * latents + at : b * latents + at + 32, :] = norm_rows(z[b, at : at + 32, :].astype(F32), g1[...])

    def item(ref, b):
        return ref[latents * b : latents * (b + 1), :]

    def project(b):
        khead[latents * b : latents * (b + 1), :] = dot_t(item(normed, b), wqkv[1]).astype(BF16)
        vhead[latents * b : latents * (b + 1), :] = dot_t(item(normed, b), wqkv[2]).astype(BF16)

    def attend(b):
        q_rows = q_all[16 * b : 16 * (b + 1)].astype(BF16)
        probs = softmax(dot_t(q_rows, item(khead, b)) * q_rows.shape[1] ** -0.5)
        context = dot(probs, item(vhead, b)).astype(BF16)
        return dot(context, wo[...])

    pair, sent1 = [], []

    def give(b, part):
        half[b] = part[8:].astype(BF16)
        pair.append(remote(half.at[b], taken.at[b], pair_sem.at[b], partner))

    def spread(b, part):
        pair[b].wait_recv()
        part1[b, xc] = (part[:8] + taken[b].astype(F32)).astype(BF16)
        sent1.append([remote(part1.at[b, xc], part1.at[b, xc], x_sem.at[0, b, d], x_peer[d]) for d in range(3)])

    for copy in load_g + load_z[:1]:
        copy.wait()
    norm_item(0)
    for copy in load_q + load_z[1:] + load_zr + load_r[:1]:
        copy.wait()
    load_dq = [load(q_hbm.at[:, pl.ds(pl.multiple_of(core * mine, mine), mine), :], queries), load(dwq_hbm, dwq)]
    chans = q_hbm.shape[2]
    load_kv = [load(dwk_hbm, dwkv.at[:, :chans]), load(dwv_hbm, dwkv.at[:, chans:])]
    load_dec = [load(dwo_hbm, dwo), load(dup_hbm, dup), load(ddn_hbm, ddn)]
    load_first = load(wout_hbm.at[:, : first.shape[1]], first)
    chip_rows = jnp.concatenate([zr[i, b].astype(F32) for b in range(items) for i in range(2)], axis=0)
    q_all = dot_t(norm_rows(chip_rows, g1[...]), wqkv[0])
    project(0)
    norm_item(1)
    parts = [attend(0)]
    project(1)
    norm_item(2)
    pl.semaphore_wait(barrier, len(peers))
    give(0, parts[0])
    parts.append(attend(1))
    project(2)
    give(1, parts[1])
    spread(0, parts[0])
    parts.append(attend(2))
    give(2, parts[2])
    spread(1, parts[1])
    for copy in load_r[1:]:
        copy.wait()
    swap_r = remote(wmlp.at[0], wmlp.at[1], pair_sem.at[items], partner)
    spread(2, parts[2])

    for copy in load_dq:
        copy.wait()
    for b in range(items):
        qd[b] = dot(norm_rows(queries[b].astype(F32), gq[...]), dwq[...]).astype(BF16)

    def gather_sum(part, b):
        total = part[b, 0].astype(F32)
        for s in range(1, 4):
            total = total + part[b, s].astype(F32)
        return total

    sent2, z_mid = [], []
    for b in range(items):
        for copy in sent1[b]:
            copy.wait_recv()
        if b == 0:
            swap_r.wait_recv()
        z_mid.append((zr[0, b].astype(F32) + gather_sum(part1, b)).astype(BF16))
        normed_mid = norm_rows(z_mid[b].astype(F32), g2[...])
        mlp = jnp.zeros((8, width), F32)
        for h in range(2):
            hidden = gelu(dot_t(normed_mid, wmlp[h, 0])).astype(BF16)
            mlp = mlp + dot(hidden, wmlp[h, 1])
        part2[b, xc] = mlp.astype(BF16)
        sent2.append([remote(part2.at[b, xc], part2.at[b, xc], x_sem.at[1, b, d], x_peer[d]) for d in range(3)])

    for copy in load_kv:
        copy.wait()
    k1, v1 = [], []
    for b in range(items):
        for copy in sent2[b]:
            copy.wait_recv()
        z_new = (z_mid[b].astype(F32) + gather_sum(part2, b)).astype(BF16)
        kv_in = norm_rows(z_new.astype(F32), gkv[...])
        both = dot(kv_in, dwkv[...])
        kbuf[b, core, zc, yc] = both[:, :chans].astype(BF16)
        vbuf[b, core, zc, yc] = both[:, chans:].astype(BF16)
        k1.append([remote(kbuf.at[b, core, zc, yc], kbuf.at[b, core, zc, yc], k1_sem.at[b, d], y_peer[d]) for d in range(3)])
        v1.append([remote(vbuf.at[b, core, zc, yc], vbuf.at[b, core, zc, yc], v1_sem.at[b, d], z_peer[d]) for d in range(3)])

    for copy in load_dec:
        copy.wait()
    k2, v2, k3, v3 = [], [], [], []

    def forward_k(b, at, i):
        k3[b].append(remote(kbuf.at[b, core, at], kbuf.at[b, core, at], k3_sem.at[b, i], partner))

    def forward_v(b, at, i):
        v3[b].append(remote(vbuf.at[b, core, :, at], vbuf.at[b, core, :, at], v3_sem.at[b, i], partner))

    for b in range(items):
        k3.append([])
        v3.append([])
        for copy in k1[b]:
            copy.wait_recv()
        k2.append([remote(kbuf.at[b, core, zc], kbuf.at[b, core, zc], k2_sem.at[b, d], z_peer[d]) for d in range(3)])
        for copy in v1[b]:
            copy.wait_recv()
        v2.append([remote(vbuf.at[b, core, :, yc], vbuf.at[b, core, :, yc], v2_sem.at[b, d], y_peer[d]) for d in range(3)])
        forward_k(b, zc, 3)
        forward_v(b, yc, 3)

    def swap(b):
        for d in (0, 2, 1):
            k2[b][d].wait_recv()
            forward_k(b, (zc + 3 - d) % 4, d)
            v2[b][d].wait_recv()
            forward_v(b, (yc + 3 - d) % 4, d)

    mixes, shared = [], []
    channels = qd.shape[2]

    def decode_first(b):
        q_item = qd[b]
        for copy in k3[b]:
            copy.wait_recv()
        keys = kbuf[b].astype(F32).reshape(latents, channels).astype(BF16)
        probs = softmax(dot_t(q_item, keys) * channels**-0.5)
        for copy in v3[b]:
            copy.wait_recv()
        values = vbuf[b].astype(F32).reshape(latents, channels).astype(BF16)
        context = dot(probs, values).astype(BF16)
        mixes.append((q_item.astype(F32) + dot(context, dwo[...])).astype(BF16))

    def decode_last(b):
        mixed = mixes[b]
        hidden = gelu(dot(norm_rows(mixed.astype(F32), gd[...]), dup[...])).astype(BF16)
        rows = pl.ds(pl.multiple_of(latents * b + core * mine, mine), mine)
        x2[rows, :] = (mixed.astype(F32) + dot(hidden, ddn[...])).astype(BF16)
        shared.append(remote(x2.at[rows], x2.at[rows], share_sem.at[b], partner))

    swap(0)
    for b in range(items):
        decode_first(b)
        if b + 1 < items:
            swap(b + 1)
        decode_last(b)

    for copy in shared:
        copy.wait_recv()
    for copy in shared + pair + [swap_r] + sum(sent1 + sent2 + k1 + v1 + k2 + v2 + k3 + v3, []):
        copy.wait_send()
    load_first.wait()


def front(latents, queries, lat_ws, dec_ws, gains, dec_out):
    items, lat_rows, width = latents.shape
    channels = queries.shape[2]
    head = lat_ws[0].shape[0]
    anywhere = pl.BlockSpec(memory_space=pl.ANY)
    total = items * lat_rows
    dma = pltpu.SemaphoreType.DMA
    return pl.pallas_call(
        front_kernel,
        out_shape=[pltpu.VMEM((total, channels), BF16), pltpu.VMEM((channels, FIRST_COLS), BF16)],
        in_specs=[anywhere] * 20,
        out_specs=[pl.BlockSpec(memory_space=pltpu.VMEM)] * 2,
        scratch_shapes=[
            pltpu.VMEM((items, lat_rows, width), BF16),
            pltpu.VMEM((2, items, 8, width), BF16),
            pltpu.VMEM((3, head, width), BF16),
            pltpu.VMEM((head, width), BF16),
            pltpu.VMEM((2, 2, head, width), BF16),
            pltpu.VMEM((items, 8, width), BF16),
            pltpu.VMEM((items, 8, width), BF16),
            pltpu.VMEM((items, lat_rows // 2, channels), BF16),
            pltpu.VMEM((channels, channels), BF16),
            pltpu.VMEM((width, 2 * channels), BF16),
            pltpu.VMEM((channels, channels), BF16),
            pltpu.VMEM((channels, channels), BF16),
            pltpu.VMEM((channels, channels), BF16),
            pltpu.VMEM((width,), F32),
            pltpu.VMEM((width,), F32),
            pltpu.VMEM((channels,), F32),
            pltpu.VMEM((width,), F32),
            pltpu.VMEM((channels,), F32),
            pltpu.VMEM((total, width), BF16),
            pltpu.VMEM((total, head), BF16),
            pltpu.VMEM((total, head), BF16),
            pltpu.VMEM((items, 4, 8, width), BF16),
            pltpu.VMEM((items, 4, 8, width), BF16),
            pltpu.VMEM((items, 2, 4, 4, 8, channels), BF16),
            pltpu.VMEM((items, 2, 4, 4, 8, channels), BF16),
            pltpu.VMEM((items, lat_rows // 2, channels), BF16),
            dma((24,)),
            dma((items + 1, 2)),
            dma((2, items, 3, 2)),
            dma((items, 3, 2)),
            dma((items, 3, 2)),
            dma((items, 3, 2)),
            dma((items, 3, 2)),
            dma((items, 4, 2)),
            dma((items, 4, 2)),
            dma((items, 2)),
        ],
        compiler_params=pltpu.CompilerParams(collective_id=0, has_side_effects=True, vmem_limit_bytes=VMEM_BYTES - HANDED),
        name="front",
    )(latents, queries, *lat_ws, *dec_ws, *gains, dec_out)


def out_kernel(plan, x2, first, wt_hbm, out_hbm, wt, out, wt_sem, out_sem):
    head, (reps, tile), tail = plan
    starts = [sum(head[:t]) for t in range(len(head))]
    base = sum(head)
    ends = [base + reps * tile + sum(tail[:t]) for t in range(len(tail))]
    fixed = list(zip(starts, head)), list(zip(ends, tail))
    steps = len(head) + reps + len(tail)

    def place(i):
        if isinstance(i, int):
            if i < len(head):
                return fixed[0][i]
            if i >= len(head) + reps:
                return fixed[1][i - len(head) - reps]
        return base + (i - len(head)) * tile, tile

    def fetch(i):
        at, width = place(i)
        at = pl.multiple_of(at, 128)
        return pltpu.make_async_copy(wt_hbm.at[:, pl.ds(at, width)], wt.at[i % 2, :, :width], wt_sem.at[i % 2])

    def store(i):
        at, width = place(i)
        at = pl.multiple_of(at, 128)
        return pltpu.make_async_copy(out.at[i % 2, :, :width], out_hbm.at[:, pl.ds(at, width)], out_sem.at[i % 2])

    def product(i):
        width = place(i)[1]
        for at in range(0, x2.shape[0], 384):
            weights = first[...] if isinstance(i, int) and i == 0 else wt[i % 2, :, :width]
            out[i % 2, at : at + 384, :width] = dot(x2[at : at + 384, :], weights).astype(BF16)

    def one(i):
        if i + 1 < steps:
            fetch(i + 1).start()
        if i:
            fetch(i).wait()
        if i >= 2:
            store(i - 2).wait()
        product(i)
        store(i).start()

    for i in range(len(head)):
        one(i)
    lo, hi = len(head), len(head) + reps

    def step(i, carry):
        @pl.when(i + 1 < hi)
        def _():
            fetch(i + 1).start()

        @pl.when(i + 1 == hi)
        def _():
            fetch(hi).start()

        fetch(i).wait()
        for t in (lo, lo + 1):
            @pl.when(i == t)
            def _(t=t):
                store(t - 2).wait()

        @pl.when(i >= lo + 2)
        def _():
            store(i - 2).wait()

        product(i)
        store(i).start()
        return carry

    lax.fori_loop(lo, hi, step, 0)
    for i in range(hi, steps):
        one(i)
    store(steps - 2).wait()
    store(steps - 1).wait()


def out_product(x2, first, dec_out):
    rows, channels = x2.shape
    cols = dec_out.shape[1]
    tile = 4096
    head, tail = (FIRST_COLS, 3072), (1792, 512)
    plan = (head, ((cols - sum(head) - sum(tail)) // tile, tile), tail)
    anywhere = pl.BlockSpec(memory_space=pl.ANY)
    dma = pltpu.SemaphoreType.DMA
    return pl.pallas_call(
        functools.partial(out_kernel, plan),
        in_specs=[pl.BlockSpec(memory_space=pltpu.VMEM)] * 2 + [anywhere],
        out_specs=anywhere,
        out_shape=jax.ShapeDtypeStruct((rows, cols), BF16),
        scratch_shapes=[
            pltpu.VMEM((2, channels, tile), BF16),
            pltpu.VMEM((2, rows, tile), BF16),
            dma((2,)),
            dma((2,)),
        ],
        compiler_params=pltpu.CompilerParams(vmem_limit_bytes=40 * 2**20),
        name="out_product",
    )(x2, first, dec_out)


def solution(mesh):
    head_split = P(None, "tp", None)
    whole_vec = P(None)
    whole_mat = P(None, None)
    in_specs = (P("dp", None, None), P("dp", "sp", None), whole_vec, head_split, head_split, head_split, P("tp", None, None), whole_vec, P(None, "tp"), P("tp", None), whole_vec, whole_vec, whole_mat, whole_mat, whole_mat, whole_mat, whole_vec, whole_mat, whole_mat, whole_mat)

    def local_step(latents, queries, lat_ln1, lat_wq, lat_wk, lat_wv, lat_wo, lat_ln2, lat_up, lat_down, dec_lnq, dec_lnkv, dec_wq, dec_wk, dec_wv, dec_wo, dec_ln, dec_up, dec_down, dec_out):
        lat_ws = [wt[:, 0, :].T for wt in (lat_wq, lat_wk, lat_wv)] + [lat_wo[0], lat_up.T, lat_down]
        gains = [lat_ln1, lat_ln2, dec_lnq, dec_lnkv, dec_ln]
        x2, first = front(latents, queries, lat_ws, [dec_wq, dec_wk, dec_wv, dec_wo, dec_up, dec_down], gains, dec_out)
        out = out_product(x2, first, dec_out)
        return out.reshape(queries.shape[0], queries.shape[1], dec_out.shape[1])

    return jax.shard_map(local_step, mesh=mesh, in_specs=in_specs, out_specs=P("dp", "sp", None), check_vma=False)
```
